256 devices in a mesh: row: 8 (over y_hi, x), col: 32 (over z, y_lo, core).
Axes of the slice: x: 4, y: 4 (y_hi: 2, y_lo: 2; y = y_hi * 2 + y_lo), z: 8, core: 2. Of those that a mesh axis runs over, the one named last changes fastest.
Arguments:
- legendre: bfloat16 [512, 512, 512], P('row', 'col'), may hold values from -6 to 6
- vectors: bfloat16 [512, 512, 256], P('row', 'col'), may hold values from -6 to 6
- panel_orders: int32 [8], replicated, may hold values from 0 to 511, as said below
- cycle_span: int32 [512, 2], replicated, may hold values from 0 to 2047, as said below
- cycle_weight: float32 [512], replicated, may hold values from 0.0009765625 to 0.0029296875
Outputs:
- projected: bfloat16 [512, 8, 256], P('col', 'row')
The draws below stay inside these ranges and needn't reach their ends.
Inputs may be any that keep to these rules, and one draw needn't show every extreme that they name: `panel_orders`: the 8 entries are distinct orders; 0 and 511 are among them. `cycle_span`: in every cycle the first entry is smaller than the second.
All inputs are finite; a program needn't handle non-finite values.
Results may differ from the reference program's by a relative error of at most 0.008.
Values may be sent and summed in bfloat16 or wider, within the bound.
No kernel may reach another device: no remote copies, remote signals or barrier semaphores. Data moves between devices by JAX's collectives and lax.ppermute only.
A program may use at most 64 MiB of HBM per device.

```python
import math
import jax
import jax.numpy as jnp
from jax import lax

BAND = 512
CYCLES = 512
VECS = 256
NPHI = 2048
PANEL = 8


def draw_panel_orders(key, part):
    inner = jax.random.permutation(jax.random.fold_in(key, 11), BAND - 2) + 1
    chosen = jnp.concatenate([jnp.array([0, BAND - 1], dtype=jnp.int32), inner[:PANEL - 2].astype(jnp.int32)])
    return jax.random.permutation(jax.random.fold_in(key, 13), chosen).astype(jnp.int32)


def draw_cycle_span(key, part):
    start_key, width_key = jax.random.split(jax.random.fold_in(key, 23))
    span_start = jax.random.randint(start_key, (CYCLES,), 0, NPHI // 2)
    span_width = jax.random.randint(width_key, (CYCLES,), NPHI // 16, NPHI // 2)
    return jnp.stack([span_start, span_start + span_width], axis=1).astype(jnp.int32)


def steps_of(rng, shape, cuts, low, high):
    loudness, own = 1.0, jax.random.fold_in(rng, 6)
    for dim, shards_of in cuts:
        steps = jnp.exp(jax.random.uniform(jax.random.fold_in(own, dim), (shards_of,), jnp.float32, low / len(cuts), high / len(cuts)))
        loudness = loudness * jnp.repeat(steps, shape[dim] // shards_of).reshape([-1 if axis == dim else 1 for axis in range(len(shape))])
    return loudness


def noise(key, dims, spread, reach, pieces=(), kind=jnp.bfloat16):
    gain = steps_of(key, dims, pieces, -0.22, 0.18) if pieces else 1.0
    drawn = jax.random.normal(key, dims, jnp.float32) * spread * gain
    return jnp.minimum(jnp.maximum(drawn, -reach), reach).astype(kind)


def setup_inputs(seed: int = 0) -> dict:
    keys = jax.random.split(jax.random.key(seed), 6)
    legendre = noise(keys[0], (BAND, BAND, CYCLES), 1.0, 6.0, ((0, 8), (1, 32)))
    vectors = noise(keys[1], (BAND, BAND, VECS), 1.0, 6.0, ((0, 8), (1, 32)))
    panel_orders = draw_panel_orders(jax.random.fold_in(keys[5], 71), 0)
    cycle_span = draw_cycle_span(jax.random.fold_in(keys[5], 71), 0)
    cycle_weight = jnp.clip(jax.random.uniform(keys[4], (CYCLES,), jnp.float32, 0.0009765625, 0.0029296875), 0.0009765625, 0.0029296875)
    return dict(legendre=legendre, vectors=vectors, panel_orders=panel_orders, cycle_span=cycle_span, cycle_weight=cycle_weight)


def mask_coef(wavenumber, span_start, span_stop):
    cell_angle = 2.0 * math.pi / NPHI
    upper_sine = jnp.sin(cell_angle * ((wavenumber * span_stop) % NPHI).astype(jnp.float32))
    lower_sine = jnp.sin(cell_angle * ((wavenumber * span_start) % NPHI).astype(jnp.float32))
    half_angle = 2.0 * jnp.sin((math.pi / NPHI) * wavenumber.astype(jnp.float32))
    safe_denom = jnp.where(wavenumber == 0, jnp.ones_like(half_angle), half_angle)
    span_width = cell_angle * (span_stop - span_start).astype(jnp.float32)
    return jnp.where(wavenumber == 0, span_width, cell_angle * (upper_sine - lower_sine) / safe_denom)


def cycle_mix(first_orders, col_orders, cycle_span, cycle_weight):
    span_start = cycle_span[:, 0][None, None, :]
    span_stop = cycle_span[:, 1][None, None, :]
    order_gap = jnp.abs(first_orders[:, None] - col_orders[None, :])[:, :, None]
    order_sum = (first_orders[:, None] + col_orders[None, :])[:, :, None]
    coef_sum = mask_coef(order_gap, span_start, span_stop) + mask_coef(order_sum, span_start, span_stop)
    return 0.5 * cycle_weight[None, None, :] * coef_sum


def reference(legendre, vectors, panel_orders, cycle_span, cycle_weight):
    orders = jnp.arange(BAND, dtype=jnp.int32)
    keep_mask = orders[None, :] >= orders[:, None]
    tables = jnp.where(keep_mask[:, :, None], legendre, jnp.zeros((), jnp.bfloat16))
    panel_rows = tables[panel_orders].astype(jnp.float32)
    mix_coef = cycle_mix(panel_orders, orders, cycle_span, cycle_weight)
    order_block = 8

    def add_block(block_index, running):
        block_start = (block_index * order_block).astype(jnp.int32)
        col_tables = lax.dynamic_slice_in_dim(tables, block_start, order_block, 0)
        cycle_coef = lax.dynamic_slice_in_dim(mix_coef, block_start, order_block, 1)
        vec_block = lax.dynamic_slice_in_dim(vectors, block_start, order_block, 0)
        vec_block = vec_block.reshape(order_block * BAND, VECS).astype(jnp.float32)
        weighted = (cycle_coef[:, :, None, :] * col_tables[None].astype(jnp.float32)).astype(jnp.bfloat16)
        weighted = weighted.reshape(PANEL, order_block * BAND, CYCLES).astype(jnp.float32)
        panel_block = jnp.einsum('plj,pqj->plq', panel_rows, weighted).astype(jnp.bfloat16)
        return running + jnp.einsum('plq,qk->lpk', panel_block.astype(jnp.float32), vec_block)

    initial = jnp.zeros((BAND, PANEL, VECS), jnp.float32)
    running = lax.fori_loop(0, BAND // order_block, add_block, initial)
    return running.astype(jnp.bfloat16)
```

```python
import math

import jax
import jax.numpy as jnp
from jax import lax
from jax.experimental import pallas as pl
from jax.experimental.pallas import tpu as pltpu
from jax.sharding import Mesh, PartitionSpec as P

NPHI = 2048
CELL = 2.0 * math.pi / NPHI
ROW = ("yh", "x")
COL = ("z", "yl", "core")
PLANE = ("z", "yl")


def sine_of_angle(x):
    square = x * x
    value = jnp.float32(-1.0 / 39916800.0)
    for term in (1.0 / 362880.0, -1.0 / 5040.0, 1.0 / 120.0, -1.0 / 6.0, 1.0):
        value = value * square + jnp.float32(term)
    return value * x


def sine_of_cells(cells):
    shifted = cells + NPHI // 4
    centred = (shifted & (NPHI // 2 - 1)) - NPHI // 4
    value = sine_of_angle(centred.astype(jnp.float32) * jnp.float32(CELL))
    return jnp.where((shifted & (NPHI // 2)) == 0, value, -value)


def half_denominator(wavenumber):
    angle = wavenumber.astype(jnp.float32) * jnp.float32(math.pi / NPHI)
    sine = 2.0 * sine_of_angle(angle)
    zero = wavenumber == 0
    return jnp.where(zero, 0.0, jnp.float32(CELL) / jnp.where(zero, 1.0, sine))


def split_kernel(orders_ref, leg_ref, vec_ref, keep_ref, send_ref, turned_ref, picks_ref):
    step = pl.program_id(0)
    block, degrees, cycles = leg_ref.shape
    half = cycles // 2
    core = lax.axis_index("core")
    row = lax.axis_index(ROW)
    first_degree = lax.axis_index(COL) * degrees
    first_order = (row * pl.num_programs(0) + step) * block
    own = pl.ds(pl.multiple_of(core * half, half), half)
    other = pl.ds(pl.multiple_of((1 - core) * half, half), half)
    gap = lax.broadcasted_iota(jnp.int32, (degrees, half), 0) + (first_degree - first_order)
    for i in range(block):
        kept = gap >= i
        keep_ref[i] = jnp.where(kept, leg_ref[i, :, own].astype(jnp.float32), 0.0).astype(jnp.bfloat16)
        send_ref[i] = jnp.where(kept, leg_ref[i, :, other].astype(jnp.float32), 0.0).astype(jnp.bfloat16)
    turned_ref[...] = vec_ref[...].reshape(block * degrees, vec_ref.shape[2]).T

    @pl.when(step == 0)
    def _():
        picks_ref[...] = jnp.zeros_like(picks_ref)

    for p in range(picks_ref.shape[0]):
        place = orders_ref[p] - first_order

        @pl.when((place >= 0) & (place < block))
        def _():
            at = jnp.clip(place, 0, block - 1)
            picks_ref[p, :, :half] = keep_ref[at]
            picks_ref[p, :, half:] = send_ref[at]


def coef_kernel(orders_ref, span_ref, weight_ref, coef_ref):
    panels, orders, half = coef_ref.shape
    own = pl.ds(pl.multiple_of(lax.axis_index("core") * half, half), half)
    start, stop = span_ref[0:1, own], span_ref[1:2, own]
    weight = 0.5 * weight_ref[0:1, own]
    first_order = lax.axis_index(ROW) * orders
    order = lax.broadcasted_iota(jnp.int32, (orders, half), 0) + first_order
    quarter = NPHI // 4
    sin_stop, cos_stop = sine_of_cells(order * stop), sine_of_cells(order * stop + quarter)
    sin_start, cos_start = sine_of_cells(order * start), sine_of_cells(order * start + quarter)
    width = weight * (jnp.float32(CELL) * (stop - start).astype(jnp.float32))
    column = lax.broadcasted_iota(jnp.int32, (orders, 128), 0) + first_order
    for p in range(panels):
        panel = orders_ref[p]
        panel_stop, panel_start = panel * stop, panel * start
        a = weight * sine_of_cells(panel_stop)
        b = weight * sine_of_cells(panel_start)
        c = weight * sine_of_cells(panel_stop + quarter)
        d = weight * sine_of_cells(panel_start + quarter)
        over_sum, over_gap = half_denominator(panel + column), half_denominator(panel - column)
        even = (over_sum + over_gap)[:, :1]
        odd = (over_sum - over_gap)[:, :1]
        at_zero = jnp.where(panel == column, 1.0, 0.0) + jnp.where(panel + column == 0, 1.0, 0.0)
        coef_ref[p] = (
            even * (a * cos_stop - b * cos_start)
            + odd * (c * sin_stop - d * sin_start)
            + at_zero[:, :1] * width
        )


def panel_kernel(coef_ref, own_t_ref, other_t_ref, own_v_ref, other_v_ref, out_ref):
    panels, orders, half = coef_ref.shape
    degrees = own_t_ref.shape[1]
    block = 256 // degrees

    def per_panel(p, carry):
        total = None
        for t_ref, v_ref in ((own_t_ref, own_v_ref), (other_t_ref, other_v_ref)):
            for first in range(0, orders, block):
                rows = []
                for o in range(first, first + block):
                    coef = jnp.broadcast_to(coef_ref[p, pl.ds(o, 1), :], (degrees, half))
                    rows.append(coef.astype(jnp.bfloat16) * t_ref[o])
                weighted = jnp.concatenate(rows, axis=0)
                columns = slice(first * degrees, (first + block) * degrees)
                part = jnp.dot(v_ref[:, columns], weighted, preferred_element_type=jnp.float32)
                total = part if total is None else total + part
        out_ref[p] = total.astype(jnp.bfloat16)
        return carry

    lax.fori_loop(0, panels, per_panel, 0)


def swapped(array):
    return lax.ppermute(array, "core", [(0, 1), (1, 0)])


def per_device(legendre, vectors, panel_orders, cycle_span, cycle_weight):
    orders, degrees, cycles = legendre.shape
    vecs = vectors.shape[2]
    panels = panel_orders.shape[0]
    half = cycles // 2
    pairs = orders * degrees
    vmem = pl.BlockSpec(memory_space=pltpu.VMEM)
    smem = pl.BlockSpec(memory_space=pltpu.SMEM)
    bf16 = jnp.bfloat16
    block = 16
    params = pltpu.CompilerParams(vmem_limit_bytes=24 * 1024 * 1024)

    with jax.named_scope("split"):
        keep, send, turned, picks = pl.pallas_call(
            split_kernel,
            grid=(orders // block,),
            in_specs=[
                smem,
                pl.BlockSpec((block, degrees, cycles), lambda i: (i, 0, 0)),
                pl.BlockSpec((block, degrees, vecs), lambda i: (i, 0, 0)),
            ],
            out_specs=[
                pl.BlockSpec((block, degrees, half), lambda i: (i, 0, 0)),
                pl.BlockSpec((block, degrees, half), lambda i: (i, 0, 0)),
                pl.BlockSpec((vecs, block * degrees), lambda i: (0, i)),
                pl.BlockSpec((panels, degrees, cycles), lambda i: (0, 0, 0)),
            ],
            out_shape=[
                jax.ShapeDtypeStruct((orders, degrees, half), bf16),
                jax.ShapeDtypeStruct((orders, degrees, half), bf16),
                jax.ShapeDtypeStruct((vecs, pairs), bf16),
                jax.ShapeDtypeStruct((panels, degrees, cycles), bf16),
            ],
            cost_estimate=pl.CostEstimate(flops=10_000_000, bytes_accessed=3_000_000, transcendentals=0),
            compiler_params=params,
        )(panel_orders, legendre, vectors)
    with jax.named_scope("swap_tables"):
        other_tables = swapped(send)
    with jax.named_scope("swap_vectors"):
        other_turned = swapped(turned)
    with jax.named_scope("picks_row"):
        picked = lax.all_to_all(picks, ROW, 0, 0, tiled=True)

    with jax.named_scope("coef"):
        coef = pl.pallas_call(
            coef_kernel,
            in_specs=[smem, vmem, vmem],
            out_specs=vmem,
            out_shape=jax.ShapeDtypeStruct((panels, orders, half), jnp.float32),
            cost_estimate=pl.CostEstimate(flops=10_000_000, bytes_accessed=500_000, transcendentals=0),
            compiler_params=params,
        )(panel_orders, cycle_span.T, cycle_weight.reshape(1, cycles))
    with jax.named_scope("panel"):
        partial = pl.pallas_call(
            panel_kernel,
            in_specs=[vmem] * 5,
            out_specs=vmem,
            out_shape=jax.ShapeDtypeStruct((panels, vecs, half), bf16),
            cost_estimate=pl.CostEstimate(
                flops=2 * panels * vecs * half * 2 * pairs, bytes_accessed=3_500_000, transcendentals=0
            ),
            compiler_params=params,
        )(coef, keep, other_tables, turned, other_turned)

    with jax.named_scope("picks_sum"):
        rows = jnp.sum(picked.astype(jnp.float32), axis=0).astype(bf16)
        copies = jnp.broadcast_to(rows, (lax.axis_size(PLANE), degrees, cycles))
    with jax.named_scope("picks_plane"):
        panel_rows = lax.all_to_all(copies, PLANE, 0, 0, tiled=True).reshape(-1, cycles)

    with jax.named_scope("reduce_row"):
        pieces = lax.all_to_all(partial, ROW, 0, 0, tiled=True)
        own = jnp.sum(pieces.astype(jnp.float32), axis=0).astype(bf16)
    with jax.named_scope("swap_sums"):
        other = swapped(own)
    with jax.named_scope("apply"):
        dims = (((1,), (1,)), ((), ()))
        applied = lax.dot_general(panel_rows[:, :half], own, dims, preferred_element_type=jnp.float32)
        applied += lax.dot_general(panel_rows[:, half:], other, dims, preferred_element_type=jnp.float32)
        applied = applied.astype(bf16).reshape(-1, degrees, vecs)
    with jax.named_scope("reduce_plane"):
        shares = lax.all_to_all(applied, PLANE, 0, 0, tiled=True)
        result = jnp.sum(shares.astype(jnp.float32), axis=0).astype(bf16)
    return result[:, None, :]


def solution(mesh):
    axes = Mesh(mesh.devices.reshape(2, 4, 8, 2, 2), ROW + COL)
    in_specs = (P(ROW, COL, None), P(ROW, COL, None), P(), P(), P())
    out_specs = P(COL, ROW, None)
    return jax.shard_map(per_device, mesh=axes, in_specs=in_specs, out_specs=out_specs, check_vma=False)
```

```python
import math

import jax
import jax.numpy as jnp
from jax import lax
from jax.experimental import pallas as pl
from jax.experimental.pallas import tpu as pltpu
from jax.sharding import Mesh, PartitionSpec as P


NPHI = 2048
CELL = 2.0 * math.pi / NPHI
ROW = ("yh", "x")
COL = ("z", "yl", "core")
PLANE = ("z", "yl")


def sine_of_angle(x):
    square = x * x
    value = jnp.float32(-1.0 / 39916800.0)
    for term in (1.0 / 362880.0, -1.0 / 5040.0, 1.0 / 120.0, -1.0 / 6.0, 1.0):
        value = value * square + jnp.float32(term)
    return value * x


def sine_of_cells(cells):
    shifted = cells + NPHI // 4
    centred = (shifted & (NPHI // 2 - 1)) - NPHI // 4
    value = sine_of_angle(centred.astype(jnp.float32) * jnp.float32(CELL))
    return jnp.where((shifted & (NPHI // 2)) == 0, value, -value)


def half_denominator(wavenumber):
    angle = wavenumber.astype(jnp.float32) * jnp.float32(math.pi / NPHI)
    sine = 2.0 * sine_of_angle(angle)
    zero = wavenumber == 0
    return jnp.where(zero, 0.0, jnp.float32(CELL) / jnp.where(zero, 1.0, sine))


def picks_kernel(orders_ref, leg_ref, picks_ref, rows, sems):
    panels, degrees, cycles = picks_ref.shape
    half = cycles // 2
    first_order = lax.axis_index(ROW) * leg_ref.shape[0]
    core = lax.axis_index("core")
    first_degree = lax.axis_index(COL) * degrees
    own = pl.ds(pl.multiple_of(core * half, half), half)
    other = pl.ds(pl.multiple_of((1 - core) * half, half), half)
    copies = []
    for p in range(panels):
        at = jnp.clip(orders_ref[p] - first_order, 0, leg_ref.shape[0] - 1)
        copies.append(pltpu.make_async_copy(leg_ref.at[at], rows.at[p], sems.at[p]))
        copies[-1].start()
    degree = lax.broadcasted_iota(jnp.int32, (degrees, half), 0) + first_degree
    for p in range(panels):
        copies[p].wait()
        place = orders_ref[p] - first_order
        held = (place >= 0) & (place < leg_ref.shape[0])
        kept = degree >= jnp.where(held, orders_ref[p], leg_ref.shape[0] * lax.axis_size(ROW))
        for lanes, part in ((own, slice(0, half)), (other, slice(half, cycles))):
            picks_ref[p, :, part] = jnp.where(kept, rows[p, :, lanes].astype(jnp.float32), 0.0).astype(jnp.bfloat16)


def coef_kernel(orders_ref, span_ref, weight_ref, coef_ref):
    panels, orders, half = coef_ref.shape
    own = pl.ds(pl.multiple_of(lax.axis_index("core") * half, half), half)
    start, stop = span_ref[0:1, own], span_ref[1:2, own]
    weight = 0.5 * weight_ref[0:1, own]
    first_order = lax.axis_index(ROW) * orders
    order = lax.broadcasted_iota(jnp.int32, (orders, half), 0) + first_order
    quarter = NPHI // 4
    sin_stop, cos_stop = sine_of_cells(order * stop), sine_of_cells(order * stop + quarter)
    sin_start, cos_start = sine_of_cells(order * start), sine_of_cells(order * start + quarter)
    width = weight * (jnp.float32(CELL) * (stop - start).astype(jnp.float32))
    column = lax.broadcasted_iota(jnp.int32, (orders, 128), 0) + first_order
    for p in range(panels):
        panel = orders_ref[p]
        panel_stop, panel_start = panel * stop, panel * start
        a = weight * sine_of_cells(panel_stop)
        b = weight * sine_of_cells(panel_start)
        c = weight * sine_of_cells(panel_stop + quarter)
        d = weight * sine_of_cells(panel_start + quarter)
        over_sum, over_gap = half_denominator(panel + column), half_denominator(panel - column)
        even = (over_sum + over_gap)[:, :1]
        odd = (over_sum - over_gap)[:, :1]
        at_zero = jnp.where(panel == column, 1.0, 0.0) + jnp.where(panel + column == 0, 1.0, 0.0)
        coef_ref[p] = (
            even * (a * cos_stop - b * cos_start)
            + odd * (c * sin_stop - d * sin_start)
            + at_zero[:, :1] * width
        )


def panel_kernel(coef_ref, own_t_ref, other_t_ref, own_v_ref, other_v_ref, out_ref, tables, turned):
    panels, orders, half = coef_ref.shape
    degrees, vecs = own_v_ref.shape[1:]
    block = 256 // degrees
    core = lax.axis_index("core")
    lanes = pl.ds(pl.multiple_of(core * half, half), half)
    first_order = lax.axis_index(ROW) * orders
    pair_degree = lax.axis_index(PLANE) * (2 * degrees)
    degree = lax.broadcasted_iota(jnp.int32, (degrees, half), 0)
    for side, (t_ref, v_ref) in enumerate(((own_t_ref, own_v_ref), (other_t_ref, other_v_ref))):
        offset = core if side == 0 else 1 - core
        gap = degree + (pair_degree + offset * degrees - first_order)

        def prepare(step, carry, side=side, t_ref=t_ref, v_ref=v_ref, gap=gap):
            start = pl.multiple_of(step * block, block)
            for i in range(block):
                table = t_ref[start + i, :, lanes].astype(jnp.float32)
                tables[side, start + i] = jnp.where(gap - start >= i, table, 0.0).astype(jnp.bfloat16)
            columns = pl.ds(pl.multiple_of(step * block * degrees, block * degrees), block * degrees)
            turned[side, :, columns] = v_ref[pl.ds(start, block)].reshape(block * degrees, vecs).T
            return carry

        lax.fori_loop(0, orders // block, prepare, 0)

    def per_panel(p, carry):
        total = None
        for side in range(2):
            for first in range(0, orders, block):
                rows = []
                for o in range(first, first + block):
                    coef = jnp.broadcast_to(coef_ref[p, pl.ds(o, 1), :], (degrees, half))
                    rows.append(coef.astype(jnp.bfloat16) * tables[side, o])
                weighted = jnp.concatenate(rows, axis=0)
                columns = slice(first * degrees, (first + block) * degrees)
                part = jnp.dot(turned[side, :, columns], weighted, preferred_element_type=jnp.float32)
                total = part if total is None else total + part
        out_ref[p] = total.astype(jnp.bfloat16)
        return carry

    lax.fori_loop(0, panels, per_panel, 0)


def join_kernel(own_ref, other_ref, out_ref):
    yl = lax.axis_index("yl")
    out_ref[yl] = own_ref[...]
    out_ref[1 - yl] = other_ref[...]


def place_kernel(*refs):
    *row_refs, out_ref = refs
    count = len(row_refs)
    degrees = row_refs[0].shape[1]
    z = lax.axis_index("z")
    for distance, row_ref in enumerate(row_refs):
        origin = lax.rem(z + (count - distance), count)
        for yl in range(2):
            at = pl.multiple_of((origin * 2 + yl) * degrees, degrees)
            out_ref[pl.ds(at, degrees), :] = row_ref[yl]


def apply_kernel(rows_ref, own_ref, other_ref, out_ref):
    half = own_ref.shape[1]
    dims = (((1,), (1,)), ((), ()))
    applied = lax.dot_general(rows_ref[:, :half], own_ref[...], dims, preferred_element_type=jnp.float32)
    applied += lax.dot_general(rows_ref[:, half:], other_ref[...], dims, preferred_element_type=jnp.float32)
    out_ref[...] = applied.astype(jnp.bfloat16).reshape(out_ref.shape)


def swapped(array):
    return lax.ppermute(array, "core", [(0, 1), (1, 0)])


def stages(legendre, vectors, panel_orders, cycle_span, cycle_weight):
    orders, degrees, cycles = legendre.shape
    vecs = vectors.shape[2]
    panels = panel_orders.shape[0]
    half = cycles // 2
    pairs = orders * degrees
    vmem = pl.BlockSpec(memory_space=pltpu.VMEM)
    smem = pl.BlockSpec(memory_space=pltpu.SMEM)
    bf16 = jnp.bfloat16
    params = pltpu.CompilerParams(vmem_limit_bytes=24 * 1024 * 1024)

    other_tables = swapped(legendre)
    other_vectors = swapped(vectors)
    picks = pl.pallas_call(
        picks_kernel,
        in_specs=[smem, pl.BlockSpec(memory_space=pltpu.HBM)],
        out_specs=vmem,
        out_shape=jax.ShapeDtypeStruct((panels, degrees, cycles), bf16),
        scratch_shapes=[
            pltpu.VMEM((panels, degrees, cycles), bf16),
            pltpu.SemaphoreType.DMA((panels,)),
        ],
        cost_estimate=pl.CostEstimate(flops=1_000_000, bytes_accessed=400_000, transcendentals=0),
        compiler_params=params,
    )(panel_orders, legendre)
    picked = lax.all_to_all(picks, ROW, 0, 0, tiled=True)

    coef = pl.pallas_call(
        coef_kernel,
        in_specs=[smem, vmem, vmem],
        out_specs=vmem,
        out_shape=jax.ShapeDtypeStruct((panels, orders, half), jnp.float32),
        cost_estimate=pl.CostEstimate(flops=10_000_000, bytes_accessed=500_000, transcendentals=0),
        compiler_params=params,
    )(panel_orders, cycle_span.T, cycle_weight.reshape(1, cycles))
    partial = pl.pallas_call(
        panel_kernel,
        in_specs=[vmem] * 5,
        out_specs=vmem,
        out_shape=jax.ShapeDtypeStruct((panels, vecs, half), bf16),
        scratch_shapes=[
            pltpu.VMEM((2, orders, degrees, half), bf16),
            pltpu.VMEM((2, vecs, pairs), bf16),
        ],
        cost_estimate=pl.CostEstimate(
            flops=2 * panels * vecs * half * 2 * pairs, bytes_accessed=3_500_000, transcendentals=0
        ),
        compiler_params=params,
    )(coef, legendre, other_tables, vectors, other_vectors)

    rows = jnp.sum(picked.astype(jnp.float32), axis=0).astype(bf16)
    paired = lax.ppermute(rows, "yl", [(0, 1), (1, 0)])
    joined = pl.pallas_call(
        join_kernel,
        in_specs=[vmem] * 2,
        out_specs=vmem,
        out_shape=jax.ShapeDtypeStruct((2, degrees, cycles), bf16),
        cost_estimate=pl.CostEstimate(flops=100_000, bytes_accessed=64_000, transcendentals=0),
        compiler_params=params,
    )(rows, paired)
    spread = [joined]
    count = lax.axis_size("z")
    for distance in range(1, count):
        spread.append(lax.ppermute(joined, "z", [(i, (i + distance) % count) for i in range(count)]))

    shared = 2 * count * degrees
    panel_rows = pl.pallas_call(
        place_kernel,
        in_specs=[vmem] * count,
        out_specs=vmem,
        out_shape=jax.ShapeDtypeStruct((shared, cycles), bf16),
        cost_estimate=pl.CostEstimate(flops=500_000, bytes_accessed=500_000, transcendentals=0),
        compiler_params=params,
    )(*spread)

    pieces = lax.all_to_all(partial, ROW, 0, 0, tiled=True)
    own = jnp.sum(pieces.astype(jnp.float32), axis=0).astype(bf16)
    other = swapped(own)
    applied = pl.pallas_call(
        apply_kernel,
        in_specs=[vmem] * 3,
        out_specs=vmem,
        out_shape=jax.ShapeDtypeStruct((2 * count, degrees, vecs), bf16),
        cost_estimate=pl.CostEstimate(flops=2 * shared * cycles * vecs, bytes_accessed=700_000, transcendentals=0),
        compiler_params=params,
    )(panel_rows, own, other)
    shares = lax.all_to_all(applied, PLANE, 0, 0, tiled=True)
    result = jnp.sum(shares.astype(jnp.float32), axis=0).astype(bf16)
    return result[:, None, :]


def solution(mesh):
    axes = Mesh(mesh.devices.reshape(2, 4, 8, 2, 2), ROW + COL)
    in_specs = (P(ROW, COL, None), P(ROW, COL, None), P(), P(), P())
    out_specs = P(COL, ROW, None)
    return jax.shard_map(stages, mesh=axes, in_specs=in_specs, out_specs=out_specs, check_vma=False)
```

```python
import math

import jax
import jax.numpy as jnp
from jax import lax
from jax.experimental import pallas as pl
from jax.experimental.pallas import tpu as pltpu
from jax.sharding import Mesh, PartitionSpec as P


NPHI = 2048
CELL = 2.0 * math.pi / NPHI
ROW = ("yh", "x")
COL = ("z", "yl", "core")
PLANE = ("z", "yl")
ROW_PAIR = ("yh", "x", "yl")


def sine_of_angle(x):
    square = x * x
    value = jnp.float32(-1.0 / 39916800.0)
    for term in (1.0 / 362880.0, -1.0 / 5040.0, 1.0 / 120.0, -1.0 / 6.0, 1.0):
        value = value * square + jnp.float32(term)
    return value * x


def sine_of_cells(cells):
    shifted = cells + NPHI // 4
    centred = (shifted & (NPHI // 2 - 1)) - NPHI // 4
    value = sine_of_angle(centred.astype(jnp.float32) * jnp.float32(CELL))
    return jnp.where((shifted & (NPHI // 2)) == 0, value, -value)


def half_denominator(wavenumber):
    angle = wavenumber.astype(jnp.float32) * jnp.float32(math.pi / NPHI)
    sine = 2.0 * sine_of_angle(angle)
    zero = wavenumber == 0
    return jnp.where(zero, 0.0, jnp.float32(CELL) / jnp.where(zero, 1.0, sine))


def picks_kernel(orders_ref, leg_ref, picks_ref, rows, sems):
    panels, sharers, degrees, cycles = picks_ref.shape
    half = cycles // 2
    first_order = lax.axis_index(ROW) * leg_ref.shape[0]
    core = lax.axis_index("core")
    first_degree = lax.axis_index(COL) * degrees
    own = pl.ds(pl.multiple_of(core * half, half), half)
    other = pl.ds(pl.multiple_of((1 - core) * half, half), half)
    copies = []
    for p in range(panels):
        at = jnp.clip(orders_ref[p] - first_order, 0, leg_ref.shape[0] - 1)
        copies.append(pltpu.make_async_copy(leg_ref.at[at], rows.at[p], sems.at[p]))
        copies[-1].start()
    degree = lax.broadcasted_iota(jnp.int32, (degrees, half), 0) + first_degree
    for p in range(panels):
        copies[p].wait()
        place = orders_ref[p] - first_order
        held = (place >= 0) & (place < leg_ref.shape[0])
        kept = degree >= jnp.where(held, orders_ref[p], leg_ref.shape[0] * lax.axis_size(ROW))
        for lanes, part in ((own, slice(0, half)), (other, slice(half, cycles))):
            pick = jnp.where(kept, rows[p, :, lanes].astype(jnp.float32), 0.0).astype(jnp.bfloat16)
            for sharer in range(sharers):
                picks_ref[p, sharer, :, part] = pick


def coef_kernel(orders_ref, span_ref, weight_ref, coef_ref):
    panels, orders, half = coef_ref.shape
    own = pl.ds(pl.multiple_of(lax.axis_index("core") * half, half), half)
    start, stop = span_ref[0:1, own], span_ref[1:2, own]
    weight = 0.5 * weight_ref[0:1, own]
    first_order = lax.axis_index(ROW) * orders
    order = lax.broadcasted_iota(jnp.int32, (orders, half), 0) + first_order
    quarter = NPHI // 4
    sin_stop, cos_stop = sine_of_cells(order * stop), sine_of_cells(order * stop + quarter)
    sin_start, cos_start = sine_of_cells(order * start), sine_of_cells(order * start + quarter)
    width = weight * (jnp.float32(CELL) * (stop - start).astype(jnp.float32))
    column = lax.broadcasted_iota(jnp.int32, (orders, 128), 0) + first_order
    for p in range(panels):
        panel = orders_ref[p]
        panel_stop, panel_start = panel * stop, panel * start
        a = weight * sine_of_cells(panel_stop)
        b = weight * sine_of_cells(panel_start)
        c = weight * sine_of_cells(panel_stop + quarter)
        d = weight * sine_of_cells(panel_start + quarter)
        over_sum, over_gap = half_denominator(panel + column), half_denominator(panel - column)
        even = (over_sum + over_gap)[:, :1]
        odd = (over_sum - over_gap)[:, :1]
        at_zero = jnp.where(panel == column, 1.0, 0.0) + jnp.where(panel + column == 0, 1.0, 0.0)
        coef_ref[p] = (
            even * (a * cos_stop - b * cos_start)
            + odd * (c * sin_stop - d * sin_start)
            + at_zero[:, :1] * width
        )


def panel_kernel(coef_ref, own_t_ref, other_t_ref, own_v_ref, other_v_ref, out_ref, tables, turned):
    panels, orders, half = coef_ref.shape
    degrees, vecs = own_v_ref.shape[1:]
    block = 256 // degrees
    core = lax.axis_index("core")
    lanes = pl.ds(pl.multiple_of(core * half, half), half)
    first_order = lax.axis_index(ROW) * orders
    pair_degree = lax.axis_index(PLANE) * (2 * degrees)
    degree = lax.broadcasted_iota(jnp.int32, (degrees, half), 0)
    for side, (t_ref, v_ref) in enumerate(((own_t_ref, own_v_ref), (other_t_ref, other_v_ref))):
        offset = core if side == 0 else 1 - core
        gap = degree + (pair_degree + offset * degrees - first_order)

        def prepare(step, carry, side=side, t_ref=t_ref, v_ref=v_ref, gap=gap):
            start = pl.multiple_of(step * block, block)
            for i in range(block):
                table = t_ref[start + i, :, lanes].astype(jnp.float32)
                tables[side, start + i] = jnp.where(gap - start >= i, table, 0.0).astype(jnp.bfloat16)
            columns = pl.ds(pl.multiple_of(step * block * degrees, block * degrees), block * degrees)
            turned[side, :, columns] = v_ref[pl.ds(start, block)].reshape(block * degrees, vecs).T
            return carry

        lax.fori_loop(0, orders // block, prepare, 0)

    def per_panel(p, carry):
        total = None
        for side in range(2):
            for first in range(0, orders, block):
                rows = []
                for o in range(first, first + block):
                    coef = jnp.broadcast_to(coef_ref[p, pl.ds(o, 1), :], (degrees, half))
                    rows.append(coef.astype(jnp.bfloat16) * tables[side, o])
                weighted = jnp.concatenate(rows, axis=0)
                columns = slice(first * degrees, (first + block) * degrees)
                part = jnp.dot(turned[side, :, columns], weighted, preferred_element_type=jnp.float32)
                total = part if total is None else total + part
        out_ref[p] = total.astype(jnp.bfloat16)
        return carry

    lax.fori_loop(0, panels, per_panel, 0)


def join_kernel(own_ref, other_ref, out_ref):
    mine = lax.rem(lax.axis_index("z"), 2)
    out_ref[mine] = own_ref[...]
    out_ref[1 - mine] = other_ref[...]


def place_kernel(*refs):
    *row_refs, out_ref = refs
    count = len(row_refs)
    pair = lax.div(lax.axis_index("z"), 2)
    for distance, row_ref in enumerate(row_refs):
        out_ref[lax.rem(pair + (count - distance), count)] = row_ref[...]


def apply_kernel(rows_ref, own_ref, other_ref, out_ref):
    half = own_ref.shape[1]
    dims = (((1,), (1,)), ((), ()))
    applied = lax.dot_general(rows_ref[:, :half], own_ref[...], dims, preferred_element_type=jnp.float32)
    applied += lax.dot_general(rows_ref[:, half:], other_ref[...], dims, preferred_element_type=jnp.float32)
    out_ref[...] = applied.astype(jnp.bfloat16).reshape(out_ref.shape)


def swapped(array):
    return lax.ppermute(array, "core", [(0, 1), (1, 0)])


def stages(legendre, vectors, panel_orders, cycle_span, cycle_weight):
    orders, degrees, cycles = legendre.shape
    vecs = vectors.shape[2]
    panels = panel_orders.shape[0]
    half = cycles // 2
    pairs = orders * degrees
    vmem = pl.BlockSpec(memory_space=pltpu.VMEM)
    smem = pl.BlockSpec(memory_space=pltpu.SMEM)
    bf16 = jnp.bfloat16
    params = pltpu.CompilerParams(vmem_limit_bytes=24 * 1024 * 1024)

    other_tables = swapped(legendre)
    other_vectors = swapped(vectors)
    picks = pl.pallas_call(
        picks_kernel,
        in_specs=[smem, pl.BlockSpec(memory_space=pltpu.HBM)],
        out_specs=vmem,
        out_shape=jax.ShapeDtypeStruct((panels, lax.axis_size("yl"), degrees, cycles), bf16),
        scratch_shapes=[
            pltpu.VMEM((panels, degrees, cycles), bf16),
            pltpu.SemaphoreType.DMA((panels,)),
        ],
        cost_estimate=pl.CostEstimate(flops=1_000_000, bytes_accessed=400_000, transcendentals=0),
        compiler_params=pltpu.CompilerParams(vmem_limit_bytes=61 * 1024 * 1024),
    )(panel_orders, legendre)
    picked = lax.all_to_all(picks.reshape(-1, degrees, cycles), ROW_PAIR, 0, 0, tiled=True)

    coef = pl.pallas_call(
        coef_kernel,
        in_specs=[smem, vmem, vmem],
        out_specs=vmem,
        out_shape=jax.ShapeDtypeStruct((panels, orders, half), jnp.float32),
        cost_estimate=pl.CostEstimate(flops=10_000_000, bytes_accessed=500_000, transcendentals=0),
        compiler_params=params,
    )(panel_orders, cycle_span.T, cycle_weight.reshape(1, cycles))
    partial = pl.pallas_call(
        panel_kernel,
        in_specs=[vmem] * 5,
        out_specs=vmem,
        out_shape=jax.ShapeDtypeStruct((panels, vecs, half), bf16),
        scratch_shapes=[
            pltpu.VMEM((2, orders, degrees, half), bf16),
            pltpu.VMEM((2, vecs, pairs), bf16),
        ],
        cost_estimate=pl.CostEstimate(
            flops=2 * panels * vecs * half * 2 * pairs, bytes_accessed=3_500_000, transcendentals=0
        ),
        compiler_params=params,
    )(coef, legendre, other_tables, vectors, other_vectors)

    rows = jnp.sum(picked.reshape(picks.shape).astype(jnp.float32), axis=0).astype(bf16)
    count = lax.axis_size("z")
    paired = lax.ppermute(rows, "z", [(i, i ^ 1) for i in range(count)])
    joined = pl.pallas_call(
        join_kernel,
        in_specs=[vmem] * 2,
        out_specs=vmem,
        out_shape=jax.ShapeDtypeStruct((2, *rows.shape), bf16),
        cost_estimate=pl.CostEstimate(flops=100_000, bytes_accessed=128_000, transcendentals=0),
        compiler_params=params,
    )(rows, paired)
    spread = [joined]
    for distance in range(2, count, 2):
        spread.append(lax.ppermute(joined, "z", [(i, (i + distance) % count) for i in range(count)]))
    panel_rows = pl.pallas_call(
        place_kernel,
        in_specs=[vmem] * len(spread),
        out_specs=vmem,
        out_shape=jax.ShapeDtypeStruct((len(spread), *joined.shape), bf16),
        cost_estimate=pl.CostEstimate(flops=500_000, bytes_accessed=500_000, transcendentals=0),
        compiler_params=params,
    )(*spread).reshape(-1, cycles)

    pieces = lax.all_to_all(partial, ROW, 0, 0, tiled=True)
    own = jnp.sum(pieces.astype(jnp.float32), axis=0).astype(bf16)
    other = swapped(own)
    applied = pl.pallas_call(
        apply_kernel,
        in_specs=[vmem] * 3,
        out_specs=vmem,
        out_shape=jax.ShapeDtypeStruct((2 * count, degrees, vecs), bf16),
        cost_estimate=pl.CostEstimate(flops=2 * panel_rows.size * vecs, bytes_accessed=700_000, transcendentals=0),
        compiler_params=params,
    )(panel_rows, own, other)
    shares = lax.all_to_all(applied, PLANE, 0, 0, tiled=True)
    result = jnp.sum(shares.astype(jnp.float32), axis=0).astype(bf16)
    return result[:, None, :]


def solution(mesh):
    axes = Mesh(mesh.devices.reshape(2, 4, 8, 2, 2), ROW + COL)
    in_specs = (P(ROW, COL, None), P(ROW, COL, None), P(), P(), P())
    out_specs = P(COL, ROW, None)
    return jax.shard_map(stages, mesh=axes, in_specs=in_specs, out_specs=out_specs, check_vma=False)
```

```python
import math

import jax
import jax.numpy as jnp
from jax import lax
from jax.experimental import pallas as pl
from jax.experimental.pallas import tpu as pltpu
from jax.sharding import Mesh, PartitionSpec as P


NPHI = 2048
CELL = 2.0 * math.pi / NPHI
ROW = ("yh", "x")
COL = ("z", "yl", "core")
PLANE = ("z", "yl")
ROW_PAIR = ("yh", "x", "yl")


def sine_of_angle(x):
    square = x * x
    value = jnp.float32(-1.0 / 39916800.0)
    for term in (1.0 / 362880.0, -1.0 / 5040.0, 1.0 / 120.0, -1.0 / 6.0, 1.0):
        value = value * square + jnp.float32(term)
    return value * x


def sine_of_cells(cells):
    shifted = cells + NPHI // 4
    centred = (shifted & (NPHI // 2 - 1)) - NPHI // 4
    value = sine_of_angle(centred.astype(jnp.float32) * jnp.float32(CELL))
    return jnp.where((shifted & (NPHI // 2)) == 0, value, -value)


def half_denominator(wavenumber):
    angle = wavenumber.astype(jnp.float32) * jnp.float32(math.pi / NPHI)
    sine = 2.0 * sine_of_angle(angle)
    zero = wavenumber == 0
    return jnp.where(zero, 0.0, jnp.float32(CELL) / jnp.where(zero, 1.0, sine))


def front_kernel(orders_ref, span_ref, weight_ref, leg_ref, picks_ref, coef_ref, rows, sides, sems):
    panels, sharers, degrees, cycles = picks_ref.shape
    orders, half = coef_ref.shape[1:]
    first_order = lax.axis_index(ROW) * orders
    core = lax.axis_index("core")
    own = pl.ds(pl.multiple_of(core * half, half), half)
    other = pl.ds(pl.multiple_of((1 - core) * half, half), half)
    places = [jnp.clip(orders_ref[p] - first_order, 0, orders - 1) for p in range(panels)]
    copies = [pltpu.make_async_copy(leg_ref.at[places[p]], rows.at[p], sems.at[p]) for p in range(panels)]
    for copy in copies:
        copy.start()

    start, stop = span_ref[0:1, own], span_ref[1:2, own]
    weight = 0.5 * weight_ref[0:1, own]
    width = weight * (jnp.float32(CELL) * (stop - start).astype(jnp.float32))
    quarter = NPHI // 4
    sublane = lax.broadcasted_iota(jnp.int32, (panels, half), 0)
    lane = lax.broadcasted_iota(jnp.int32, (orders, 128), 1)
    panel_row, panel_lane = jnp.zeros_like(sublane), jnp.zeros_like(lane)
    for p in range(panels):
        panel_row = jnp.where(sublane == p, orders_ref[p], panel_row)
        panel_lane = jnp.where(lane == p, orders_ref[p], panel_lane)
    sides[0] = weight * sine_of_cells(panel_row * stop)
    sides[1] = weight * sine_of_cells(panel_row * start)
    sides[2] = weight * sine_of_cells(panel_row * stop + quarter)
    sides[3] = weight * sine_of_cells(panel_row * start + quarter)
    order = lax.broadcasted_iota(jnp.int32, (orders, half), 0) + first_order
    sin_stop, cos_stop = sine_of_cells(order * stop), sine_of_cells(order * stop + quarter)
    sin_start, cos_start = sine_of_cells(order * start), sine_of_cells(order * start + quarter)
    column = lax.broadcasted_iota(jnp.int32, (orders, 128), 0) + first_order
    over_sum, over_gap = half_denominator(panel_lane + column), half_denominator(panel_lane - column)
    even, odd = over_sum + over_gap, over_sum - over_gap
    for p in range(panels):
        at = slice(p, p + 1)
        coef_ref[p] = even[:, at] * (sides[0, at] * cos_stop - sides[1, at] * cos_start) + odd[:, at] * (
            sides[2, at] * sin_stop - sides[3, at] * sin_start
        )

    degree = lax.broadcasted_iota(jnp.int32, (degrees, half), 0) + lax.axis_index(COL) * degrees
    for p in range(panels):
        panel = orders_ref[p]
        held = (panel >= first_order) & (panel < first_order + orders)
        zeros = jnp.where(held, jnp.where(panel == 0, 2.0, 1.0), 0.0)
        at = pl.ds(places[p], 1)
        coef_ref[p, at, :] = coef_ref[p, at, :] + zeros * width
        copies[p].wait()
        kept = degree >= jnp.where(held, panel, orders * lax.axis_size(ROW))
        for lanes, part in ((own, slice(0, half)), (other, slice(half, cycles))):
            pick = jnp.where(kept, rows[p, :, lanes].astype(jnp.float32), 0.0).astype(jnp.bfloat16)
            for sharer in range(sharers):
                picks_ref[p, sharer, :, part] = pick


def panel_kernel(coef_ref, own_t_ref, other_t_ref, own_v_ref, other_v_ref, out_ref, tables, turned, sums, sems):
    panels, orders, half = coef_ref.shape
    degrees, vecs = own_v_ref.shape[1:]
    block = 256 // degrees
    core = lax.axis_index("core")
    lanes = pl.ds(pl.multiple_of(core * half, half), half)
    first_order = lax.axis_index(ROW) * orders
    pair_degree = lax.axis_index(PLANE) * (2 * degrees)
    degree = lax.broadcasted_iota(jnp.int32, (degrees, half), 0)
    for side, (t_ref, v_ref) in enumerate(((own_t_ref, own_v_ref), (other_t_ref, other_v_ref))):
        offset = core if side == 0 else 1 - core
        gap = degree + (pair_degree + offset * degrees - first_order)

        def prepare(step, carry, side=side, t_ref=t_ref, v_ref=v_ref, gap=gap):
            start = pl.multiple_of(step * block, block)
            for i in range(block):
                table = t_ref[start + i, :, lanes].astype(jnp.float32)
                tables[side, start + i] = jnp.where(gap - start >= i, table, 0.0).astype(jnp.bfloat16)
            columns = pl.ds(pl.multiple_of(step * block * degrees, block * degrees), block * degrees)
            turned[side, :, columns] = v_ref[pl.ds(start, block)].reshape(block * degrees, vecs).T
            return carry

        lax.fori_loop(0, orders // block, prepare, 0)

    def outgoing(p):
        return pltpu.make_async_copy(sums.at[p], out_ref.at[p], sems.at[p])

    def per_panel(p, carry):
        @pl.when(p > 0)
        def _():
            outgoing(jnp.maximum(p - 1, 0)).start()

        total = None
        for side in range(2):
            for first in range(0, orders, block):
                rows = []
                for o in range(first, first + block):
                    coef = jnp.broadcast_to(coef_ref[p, pl.ds(o, 1), :], (degrees, half))
                    rows.append(coef.astype(jnp.bfloat16) * tables[side, o])
                weighted = jnp.concatenate(rows, axis=0)
                columns = slice(first * degrees, (first + block) * degrees)
                part = jnp.dot(turned[side, :, columns], weighted, preferred_element_type=jnp.float32)
                total = part if total is None else total + part
        sums[p] = total.astype(jnp.bfloat16)
        return carry

    lax.fori_loop(0, panels, per_panel, 0)
    outgoing(panels - 1).start()
    for p in range(panels):
        outgoing(p).wait()


def join_kernel(own_ref, other_ref, out_ref):
    mine = lax.rem(lax.axis_index("z"), 2)
    out_ref[mine] = own_ref[...]
    out_ref[1 - mine] = other_ref[...]


def place_kernel(*refs):
    *row_refs, out_ref = refs
    count = len(row_refs)
    pair = lax.div(lax.axis_index("z"), 2)
    distances = sorted(range(count), key=lambda d: min(d, count - d))
    for distance, row_ref in zip(distances, row_refs):
        out_ref[lax.rem(pair + (count - distance), count)] = row_ref[...]


def apply_kernel(rows_ref, own_ref, other_ref, out_ref):
    half = own_ref.shape[1]
    dims = (((1,), (1,)), ((), ()))
    applied = lax.dot_general(rows_ref[:, :half], own_ref[...], dims, preferred_element_type=jnp.float32)
    applied += lax.dot_general(rows_ref[:, half:], other_ref[...], dims, preferred_element_type=jnp.float32)
    out_ref[...] = applied.astype(jnp.bfloat16).reshape(out_ref.shape)


def swapped(array):
    return lax.ppermute(array, "core", [(0, 1), (1, 0)])


def stages(legendre, vectors, panel_orders, cycle_span, cycle_weight):
    orders, degrees, cycles = legendre.shape
    vecs = vectors.shape[2]
    panels = panel_orders.shape[0]
    half = cycles // 2
    pairs = orders * degrees
    vmem = pl.BlockSpec(memory_space=pltpu.VMEM)
    smem = pl.BlockSpec(memory_space=pltpu.SMEM)
    bf16 = jnp.bfloat16
    params = pltpu.CompilerParams(vmem_limit_bytes=24 * 1024 * 1024)

    other_tables = swapped(legendre)
    other_vectors = swapped(vectors)
    picks, coef = pl.pallas_call(
        front_kernel,
        in_specs=[smem, vmem, vmem, pl.BlockSpec(memory_space=pltpu.HBM)],
        out_specs=[vmem, vmem],
        out_shape=[
            jax.ShapeDtypeStruct((panels, lax.axis_size("yl"), degrees, cycles), bf16),
            jax.ShapeDtypeStruct((panels, orders, half), jnp.float32),
        ],
        scratch_shapes=[
            pltpu.VMEM((panels, degrees, cycles), bf16),
            pltpu.VMEM((4, panels, half), jnp.float32),
            pltpu.SemaphoreType.DMA((panels,)),
        ],
        cost_estimate=pl.CostEstimate(flops=10_000_000, bytes_accessed=900_000, transcendentals=0),
        compiler_params=pltpu.CompilerParams(vmem_limit_bytes=60 * 1024 * 1024),
    )(panel_orders, cycle_span.T, cycle_weight.reshape(1, cycles), legendre)
    picked = lax.all_to_all(picks.reshape(-1, degrees, cycles), ROW_PAIR, 0, 0, tiled=True)

    partial = pl.pallas_call(
        panel_kernel,
        in_specs=[vmem] * 5,
        out_specs=pl.BlockSpec(memory_space=pltpu.HBM),
        out_shape=jax.ShapeDtypeStruct((panels, vecs, half), bf16),
        scratch_shapes=[
            pltpu.VMEM((2, orders, degrees, half), bf16),
            pltpu.VMEM((2, vecs, pairs), bf16),
            pltpu.VMEM((panels, vecs, half), bf16),
            pltpu.SemaphoreType.DMA((panels,)),
        ],
        cost_estimate=pl.CostEstimate(
            flops=2 * panels * vecs * half * 2 * pairs, bytes_accessed=3_500_000, transcendentals=0
        ),
        compiler_params=params,
    )(coef, legendre, other_tables, vectors, other_vectors)

    rows = jnp.sum(picked.reshape(picks.shape).astype(jnp.float32), axis=0).astype(bf16)
    count = lax.axis_size("z")
    paired = lax.ppermute(rows, "z", [(i, i ^ 1) for i in range(count)])
    joined = pl.pallas_call(
        join_kernel,
        in_specs=[vmem] * 2,
        out_specs=vmem,
        out_shape=jax.ShapeDtypeStruct((2, *rows.shape), bf16),
        cost_estimate=pl.CostEstimate(flops=100_000, bytes_accessed=128_000, transcendentals=0),
        compiler_params=params,
    )(rows, paired)
    spread = [joined]
    for distance in sorted(range(2, count, 2), key=lambda d: min(d, count - d)):
        spread.append(lax.ppermute(joined, "z", [(i, (i + distance) % count) for i in range(count)]))
    panel_rows = pl.pallas_call(
        place_kernel,
        in_specs=[vmem] * len(spread),
        out_specs=vmem,
        out_shape=jax.ShapeDtypeStruct((len(spread), *joined.shape), bf16),
        cost_estimate=pl.CostEstimate(flops=500_000, bytes_accessed=500_000, transcendentals=0),
        compiler_params=params,
    )(*spread).reshape(-1, cycles)

    pieces = lax.all_to_all(partial, ROW, 0, 0, tiled=True)
    own = jnp.sum(pieces.astype(jnp.float32), axis=0).astype(bf16)
    other = swapped(own)
    applied = pl.pallas_call(
        apply_kernel,
        in_specs=[vmem] * 3,
        out_specs=vmem,
        out_shape=jax.ShapeDtypeStruct((2 * count, degrees, vecs), bf16),
        cost_estimate=pl.CostEstimate(flops=2 * panel_rows.size * vecs, bytes_accessed=700_000, transcendentals=0),
        compiler_params=params,
    )(panel_rows, own, other)
    shares = lax.all_to_all(applied, PLANE, 0, 0, tiled=True)
    result = jnp.sum(shares.astype(jnp.float32), axis=0).astype(bf16)
    return result[:, None, :]


def solution(mesh):
    axes = Mesh(mesh.devices.reshape(2, 4, 8, 2, 2), ROW + COL)
    in_specs = (P(ROW, COL, None), P(ROW, COL, None), P(), P(), P())
    out_specs = P(COL, ROW, None)
    return jax.shard_map(stages, mesh=axes, in_specs=in_specs, out_specs=out_specs, check_vma=False)
```

```python
import math

import jax
import jax.numpy as jnp
from jax import lax
from jax.experimental import pallas as pl
from jax.experimental.pallas import tpu as pltpu
from jax.sharding import Mesh, PartitionSpec as P


NPHI = 2048
CELL = 2.0 * math.pi / NPHI
ROW = ("yh", "x")
COL = ("z", "yl", "core")
PLANE = ("z", "yl")
ROW_PAIR = ("yh", "x", "yl")


def sine_of_angle(x):
    square = x * x
    value = jnp.float32(-1.0 / 39916800.0)
    for term in (1.0 / 362880.0, -1.0 / 5040.0, 1.0 / 120.0, -1.0 / 6.0, 1.0):
        value = value * square + jnp.float32(term)
    return value * x


def sine_of_cells(cells):
    shifted = cells + NPHI // 4
    centred = (shifted & (NPHI // 2 - 1)) - NPHI // 4
    value = sine_of_angle(centred.astype(jnp.float32) * jnp.float32(CELL))
    return jnp.where((shifted & (NPHI // 2)) == 0, value, -value)


def half_denominator(wavenumber):
    angle = wavenumber.astype(jnp.float32) * jnp.float32(math.pi / NPHI)
    sine = 2.0 * sine_of_angle(angle)
    zero = wavenumber == 0
    return jnp.where(zero, 0.0, jnp.float32(CELL) / jnp.where(zero, 1.0, sine))


def picks_kernel(orders_ref, leg_ref, picks_ref, rows, sems):
    panels, sharers, degrees, cycles = picks_ref.shape
    orders = leg_ref.shape[0]
    half = cycles // 2
    first_order = lax.axis_index(ROW) * orders
    core = lax.axis_index("core")
    own = pl.ds(pl.multiple_of(core * half, half), half)
    other = pl.ds(pl.multiple_of((1 - core) * half, half), half)
    copies = []
    for p in range(panels):
        place = jnp.clip(orders_ref[p] - first_order, 0, orders - 1)
        copies.append(pltpu.make_async_copy(leg_ref.at[place], rows.at[p], sems.at[p]))
        copies[p].start()
    degree = lax.broadcasted_iota(jnp.int32, (degrees, half), 0) + lax.axis_index(COL) * degrees
    for p in range(panels):
        panel = orders_ref[p]
        held = (panel >= first_order) & (panel < first_order + orders)
        kept = degree >= jnp.where(held, panel, orders * lax.axis_size(ROW))
        copies[p].wait()
        for lanes, part in ((own, slice(0, half)), (other, slice(half, cycles))):
            pick = jnp.where(kept, rows[p, :, lanes].astype(jnp.float32), 0.0).astype(jnp.bfloat16)
            for sharer in range(sharers):
                picks_ref[p, sharer, :, part] = pick


def fill_coefs(orders_ref, span_ref, weight_ref, coefs, sides):
    panels, orders, half = coefs.shape
    first_order = lax.axis_index(ROW) * orders
    own = pl.ds(pl.multiple_of(lax.axis_index("core") * half, half), half)
    start, stop = span_ref[0:1, own], span_ref[1:2, own]
    weight = 0.5 * weight_ref[0:1, own]
    width = weight * (jnp.float32(CELL) * (stop - start).astype(jnp.float32))
    quarter = NPHI // 4
    sublane = lax.broadcasted_iota(jnp.int32, (panels, half), 0)
    lane = lax.broadcasted_iota(jnp.int32, (orders, 128), 1)
    panel_row, panel_lane = jnp.zeros_like(sublane), jnp.zeros_like(lane)
    for p in range(panels):
        panel_row = jnp.where(sublane == p, orders_ref[p], panel_row)
        panel_lane = jnp.where(lane == p, orders_ref[p], panel_lane)
    sides[0] = weight * sine_of_cells(panel_row * stop)
    sides[1] = weight * sine_of_cells(panel_row * start)
    sides[2] = weight * sine_of_cells(panel_row * stop + quarter)
    sides[3] = weight * sine_of_cells(panel_row * start + quarter)
    order = lax.broadcasted_iota(jnp.int32, (orders, half), 0) + first_order
    sin_stop, cos_stop = sine_of_cells(order * stop), sine_of_cells(order * stop + quarter)
    sin_start, cos_start = sine_of_cells(order * start), sine_of_cells(order * start + quarter)
    column = lax.broadcasted_iota(jnp.int32, (orders, 128), 0) + first_order
    over_sum, over_gap = half_denominator(panel_lane + column), half_denominator(panel_lane - column)
    even, odd = over_sum + over_gap, over_sum - over_gap
    for p in range(panels):
        at = slice(p, p + 1)
        coefs[p] = even[:, at] * (sides[0, at] * cos_stop - sides[1, at] * cos_start) + odd[:, at] * (
            sides[2, at] * sin_stop - sides[3, at] * sin_start
        )
    for p in range(panels):
        panel = orders_ref[p]
        held = (panel >= first_order) & (panel < first_order + orders)
        zeros = jnp.where(held, jnp.where(panel == 0, 2.0, 1.0), 0.0)
        at = pl.ds(jnp.clip(panel - first_order, 0, orders - 1), 1)
        coefs[p, at, :] = coefs[p, at, :] + zeros * width


def panel_kernel(orders_ref, span_ref, weight_ref, own_t_ref, other_t_ref, own_v_ref, other_v_ref, out_ref, *scratch):
    coefs, sides, tables, turned, sums, sem = scratch
    panels, orders, half = coefs.shape
    degrees, vecs = own_v_ref.shape[1:]
    block = 256 // degrees
    core = lax.axis_index("core")
    lanes = pl.ds(pl.multiple_of(core * half, half), half)
    first_order = lax.axis_index(ROW) * orders
    pair_degree = lax.axis_index(PLANE) * (2 * degrees)
    degree = lax.broadcasted_iota(jnp.int32, (degrees, half), 0)
    fill_coefs(orders_ref, span_ref, weight_ref, coefs, sides)
    blocks = []
    for t_ref, v_ref, offset in ((own_t_ref, own_v_ref, core), (other_t_ref, other_v_ref, 1 - core)):
        gap = degree + (pair_degree + offset * degrees - first_order)
        blocks += [(t_ref, v_ref, gap, first) for first in range(0, orders, block)]
    for p in range(panels):
        total = None
        for index, (t_ref, v_ref, gap, first) in enumerate(blocks):
            if p == 0:
                for i in range(block):
                    table = t_ref[first + i, :, lanes].astype(jnp.float32)
                    tables[index, i] = jnp.where(gap >= first + i, table, 0.0).astype(jnp.bfloat16)
                turned[index] = v_ref[first : first + block].reshape(block * degrees, vecs).T
            rows = []
            for i in range(block):
                coef = jnp.broadcast_to(coefs[p, pl.ds(first + i, 1), :], (degrees, half))
                rows.append(coef.astype(jnp.bfloat16) * tables[index, i])
            part = jnp.dot(turned[index], jnp.concatenate(rows, axis=0), preferred_element_type=jnp.float32)
            total = part if total is None else total + part
        sums[p] = total.astype(jnp.bfloat16)
    store = pltpu.make_async_copy(sums, out_ref, sem)
    store.start()
    store.wait()


def join_kernel(own_ref, other_ref, out_ref):
    mine = lax.rem(lax.axis_index("z"), 2)
    out_ref[mine] = own_ref[...]
    out_ref[1 - mine] = other_ref[...]


def place_kernel(*refs):
    *row_refs, out_ref = refs
    count = len(row_refs)
    pair = lax.div(lax.axis_index("z"), 2)
    distances = sorted(range(count), key=lambda d: min(d, count - d))
    for distance, row_ref in zip(distances, row_refs):
        out_ref[lax.rem(pair + (count - distance), count)] = row_ref[...]


def apply_kernel(rows_ref, own_ref, other_ref, out_ref):
    half = own_ref.shape[1]
    dims = (((1,), (1,)), ((), ()))
    applied = lax.dot_general(rows_ref[:, :half], own_ref[...], dims, preferred_element_type=jnp.float32)
    applied += lax.dot_general(rows_ref[:, half:], other_ref[...], dims, preferred_element_type=jnp.float32)
    out_ref[...] = applied.astype(jnp.bfloat16).reshape(out_ref.shape)


def swapped(array):
    return lax.ppermute(array, "core", [(0, 1), (1, 0)])


def stages(legendre, vectors, panel_orders, cycle_span, cycle_weight):
    orders, degrees, cycles = legendre.shape
    vecs = vectors.shape[2]
    panels = panel_orders.shape[0]
    half = cycles // 2
    pairs = orders * degrees
    vmem = pl.BlockSpec(memory_space=pltpu.VMEM)
    smem = pl.BlockSpec(memory_space=pltpu.SMEM)
    bf16 = jnp.bfloat16
    params = pltpu.CompilerParams(vmem_limit_bytes=24 * 1024 * 1024)

    other_tables = swapped(legendre)
    other_vectors = swapped(vectors)
    picks = pl.pallas_call(
        picks_kernel,
        in_specs=[smem, pl.BlockSpec(memory_space=pltpu.HBM)],
        out_specs=vmem,
        out_shape=jax.ShapeDtypeStruct((panels, lax.axis_size("yl"), degrees, cycles), bf16),
        scratch_shapes=[
            pltpu.VMEM((panels, degrees, cycles), bf16),
            pltpu.SemaphoreType.DMA((panels,)),
        ],
        cost_estimate=pl.CostEstimate(flops=1_000_000, bytes_accessed=400_000, transcendentals=0),
        compiler_params=pltpu.CompilerParams(vmem_limit_bytes=60 * 1024 * 1024),
    )(panel_orders, legendre)
    picked = lax.all_to_all(picks.reshape(-1, degrees, cycles), ROW_PAIR, 0, 0, tiled=True)

    partial = pl.pallas_call(
        panel_kernel,
        in_specs=[smem] + [vmem] * 6,
        out_specs=pl.BlockSpec(memory_space=pltpu.HBM),
        out_shape=jax.ShapeDtypeStruct((panels, vecs, half), bf16),
        scratch_shapes=[
            pltpu.VMEM((panels, orders, half), jnp.float32),
            pltpu.VMEM((4, panels, half), jnp.float32),
            pltpu.VMEM((2 * pairs // 256, 256 // degrees, degrees, half), bf16),
            pltpu.VMEM((2 * pairs // 256, vecs, 256), bf16),
            pltpu.VMEM((panels, vecs, half), bf16),
            pltpu.SemaphoreType.DMA,
        ],
        cost_estimate=pl.CostEstimate(
            flops=2 * panels * vecs * half * 2 * pairs, bytes_accessed=3_500_000, transcendentals=0
        ),
        compiler_params=params,
    )(
        panel_orders,
        cycle_span.T,
        cycle_weight.reshape(1, cycles),
        legendre,
        other_tables,
        vectors,
        other_vectors,
    )

    rows = jnp.sum(picked.reshape(picks.shape).astype(jnp.float32), axis=0).astype(bf16)
    count = lax.axis_size("z")
    paired = lax.ppermute(rows, "z", [(i, i ^ 1) for i in range(count)])
    joined = pl.pallas_call(
        join_kernel,
        in_specs=[vmem] * 2,
        out_specs=vmem,
        out_shape=jax.ShapeDtypeStruct((2, *rows.shape), bf16),
        cost_estimate=pl.CostEstimate(flops=100_000, bytes_accessed=128_000, transcendentals=0),
        compiler_params=params,
    )(rows, paired)
    spread = [joined]
    for distance in sorted(range(2, count, 2), key=lambda d: min(d, count - d)):
        spread.append(lax.ppermute(joined, "z", [(i, (i + distance) % count) for i in range(count)]))
    panel_rows = pl.pallas_call(
        place_kernel,
        in_specs=[vmem] * len(spread),
        out_specs=vmem,
        out_shape=jax.ShapeDtypeStruct((len(spread), *joined.shape), bf16),
        cost_estimate=pl.CostEstimate(flops=500_000, bytes_accessed=500_000, transcendentals=0),
        compiler_params=params,
    )(*spread).reshape(-1, cycles)

    pieces = lax.all_to_all(partial, ROW, 0, 0, tiled=True)
    own = jnp.sum(pieces.astype(jnp.float32), axis=0).astype(bf16)
    other = swapped(own)
    applied = pl.pallas_call(
        apply_kernel,
        in_specs=[vmem] * 3,
        out_specs=vmem,
        out_shape=jax.ShapeDtypeStruct((2 * count, degrees, vecs), bf16),
        cost_estimate=pl.CostEstimate(flops=2 * panel_rows.size * vecs, bytes_accessed=700_000, transcendentals=0),
        compiler_params=params,
    )(panel_rows, own, other)
    shares = lax.all_to_all(applied, PLANE, 0, 0, tiled=True)
    result = jnp.sum(shares.astype(jnp.float32), axis=0).astype(bf16)
    return result[:, None, :]


def solution(mesh):
    axes = Mesh(mesh.devices.reshape(2, 4, 8, 2, 2), ROW + COL)
    in_specs = (P(ROW, COL, None), P(ROW, COL, None), P(), P(), P())
    out_specs = P(COL, ROW, None)
    return jax.shard_map(stages, mesh=axes, in_specs=in_specs, out_specs=out_specs, check_vma=False)
```

```python
import math

import jax
import jax.numpy as jnp
from jax import lax
from jax.experimental import pallas as pl
from jax.experimental.pallas import tpu as pltpu
from jax.sharding import Mesh, PartitionSpec as P


NPHI = 2048
CELL = 2.0 * math.pi / NPHI
ROW = ("yh", "x")
COL = ("z", "yl", "core")
PLANE = ("z", "yl")
ROW_PAIR = ("yh", "x", "yl")


def sine_of_angle(x):
    square = x * x
    value = jnp.float32(-1.0 / 39916800.0)
    for term in (1.0 / 362880.0, -1.0 / 5040.0, 1.0 / 120.0, -1.0 / 6.0, 1.0):
        value = value * square + jnp.float32(term)
    return value * x


def sine_of_cells(cells):
    shifted = cells + NPHI // 4
    centred = (shifted & (NPHI // 2 - 1)) - NPHI // 4
    value = sine_of_angle(centred.astype(jnp.float32) * jnp.float32(CELL))
    return jnp.where((shifted & (NPHI // 2)) == 0, value, -value)


def half_denominator(wavenumber):
    angle = wavenumber.astype(jnp.float32) * jnp.float32(math.pi / NPHI)
    sine = 2.0 * sine_of_angle(angle)
    zero = wavenumber == 0
    return jnp.where(zero, 0.0, jnp.float32(CELL) / jnp.where(zero, 1.0, sine))


def picks_kernel(orders_ref, leg_ref, picks_ref, sems):
    panels, sharers = picks_ref.shape[:2]
    orders = leg_ref.shape[0]
    first_order = lax.axis_index(ROW) * orders

    def copies(p):
        place = jnp.clip(orders_ref[p] - first_order, 0, orders - 1)
        return [
            pltpu.make_async_copy(leg_ref.at[place], picks_ref.at[p, sharer], sems.at[p, sharer])
            for sharer in range(sharers)
        ]

    def held(p):
        return (orders_ref[p] >= first_order) & (orders_ref[p] < first_order + orders)

    for p in range(panels):

        @pl.when(held(p))
        def _():
            for copy in copies(p):
                copy.start()

        @pl.when(jnp.logical_not(held(p)))
        def _():
            picks_ref[p] = jnp.zeros_like(picks_ref[p])

    for p in range(panels):

        @pl.when(held(p))
        def _():
            for copy in copies(p):
                copy.wait()


def rows_kernel(orders_ref, picked_ref, rows_ref):
    sharers, degrees, cycles = rows_ref.shape
    half = cycles // 2
    core = lax.axis_index("core")
    panel = orders_ref[lax.axis_index(ROW)]
    own = pl.ds(pl.multiple_of(core * half, half), half)
    other = pl.ds(pl.multiple_of((1 - core) * half, half), half)
    for sharer in range(sharers):
        place = (lax.axis_index("z") * sharers + sharer) * lax.axis_size("core") + core
        degree = lax.broadcasted_iota(jnp.int32, (degrees, half), 0) + place * degrees
        for lanes, part in ((own, slice(0, half)), (other, slice(half, cycles))):
            total = picked_ref[sharer, :, lanes].astype(jnp.float32)
            for source in range(sharers + sharer, picked_ref.shape[0], sharers):
                total += picked_ref[source, :, lanes].astype(jnp.float32)
            rows_ref[sharer, :, part] = jnp.where(degree >= panel, total, 0.0).astype(jnp.bfloat16)


def sum_kernel(pieces_ref, out_ref):
    count, rows, _ = pieces_ref.shape
    for first in range(0, rows, 16):
        at = slice(first, first + 16)
        terms = [pieces_ref[i, at].astype(jnp.float32) for i in range(count)]
        while len(terms) > 1:
            terms = [sum(terms[i : i + 2]) for i in range(0, len(terms), 2)]
        out_ref[at] = terms[0].astype(jnp.bfloat16)


def fill_coefs(orders_ref, span_ref, weight_ref, coefs, sides):
    panels, orders, half = coefs.shape
    first_order = lax.axis_index(ROW) * orders
    own = pl.ds(pl.multiple_of(lax.axis_index("core") * half, half), half)
    start, stop = span_ref[0:1, own], span_ref[1:2, own]
    weight = 0.5 * weight_ref[0:1, own]
    width = weight * (jnp.float32(CELL) * (stop - start).astype(jnp.float32))
    quarter = NPHI // 4
    sublane = lax.broadcasted_iota(jnp.int32, (panels, half), 0)
    lane = lax.broadcasted_iota(jnp.int32, (orders, 128), 1)
    panel_row, panel_lane = jnp.zeros_like(sublane), jnp.zeros_like(lane)
    for p in range(panels):
        panel_row = jnp.where(sublane == p, orders_ref[p], panel_row)
        panel_lane = jnp.where(lane == p, orders_ref[p], panel_lane)
    sides[0] = weight * sine_of_cells(panel_row * stop)
    sides[1] = weight * sine_of_cells(panel_row * start)
    sides[2] = weight * sine_of_cells(panel_row * stop + quarter)
    sides[3] = weight * sine_of_cells(panel_row * start + quarter)
    order = lax.broadcasted_iota(jnp.int32, (orders, half), 0) + first_order
    sin_stop, cos_stop = sine_of_cells(order * stop), sine_of_cells(order * stop + quarter)
    sin_start, cos_start = sine_of_cells(order * start), sine_of_cells(order * start + quarter)
    column = lax.broadcasted_iota(jnp.int32, (orders, 128), 0) + first_order
    over_sum, over_gap = half_denominator(panel_lane + column), half_denominator(panel_lane - column)
    even, odd = over_sum + over_gap, over_sum - over_gap
    for p in range(panels):
        at = slice(p, p + 1)
        coefs[p] = even[:, at] * (sides[0, at] * cos_stop - sides[1, at] * cos_start) + odd[:, at] * (
            sides[2, at] * sin_stop - sides[3, at] * sin_start
        )
    for p in range(panels):
        panel = orders_ref[p]
        held = (panel >= first_order) & (panel < first_order + orders)
        zeros = jnp.where(held, jnp.where(panel == 0, 2.0, 1.0), 0.0)
        at = pl.ds(jnp.clip(panel - first_order, 0, orders - 1), 1)
        coefs[p, at, :] = coefs[p, at, :] + zeros * width


def panel_kernel(orders_ref, span_ref, weight_ref, own_t_ref, other_t_ref, own_v_ref, other_v_ref, out_ref, *scratch):
    coefs, sides, tables, turned, sums, sem = scratch
    panels, orders, half = coefs.shape
    degrees, vecs = own_v_ref.shape[1:]
    block = 256 // degrees
    core = lax.axis_index("core")
    lanes = pl.ds(pl.multiple_of(core * half, half), half)
    first_order = lax.axis_index(ROW) * orders
    pair_degree = lax.axis_index(PLANE) * (2 * degrees)
    degree = lax.broadcasted_iota(jnp.int32, (degrees, half), 0)
    fill_coefs(orders_ref, span_ref, weight_ref, coefs, sides)
    blocks = []
    for t_ref, v_ref, offset in ((own_t_ref, own_v_ref, core), (other_t_ref, other_v_ref, 1 - core)):
        gap = degree + (pair_degree + offset * degrees - first_order)
        blocks += [(t_ref, v_ref, gap, first) for first in range(0, orders, block)]
    for p in range(panels):
        total = None
        for index, (t_ref, v_ref, gap, first) in enumerate(blocks):
            if p == 0:
                for i in range(block):
                    table = t_ref[first + i, :, lanes].astype(jnp.float32)
                    tables[index, i] = jnp.where(gap >= first + i, table, 0.0).astype(jnp.bfloat16)
                turned[index] = v_ref[first : first + block].reshape(block * degrees, vecs).T
            rows = []
            for i in range(block):
                coef = jnp.broadcast_to(coefs[p, pl.ds(first + i, 1), :], (degrees, half))
                rows.append(coef.astype(jnp.bfloat16) * tables[index, i])
            part = jnp.dot(turned[index], jnp.concatenate(rows, axis=0), preferred_element_type=jnp.float32)
            total = part if total is None else total + part
        sums[p] = total.astype(jnp.bfloat16)
    store = pltpu.make_async_copy(sums, out_ref, sem)
    store.start()
    store.wait()


def join_kernel(own_ref, other_ref, out_ref):
    mine = lax.rem(lax.axis_index("z"), 2)
    out_ref[mine] = own_ref[...]
    out_ref[1 - mine] = other_ref[...]


def place_kernel(*refs):
    *row_refs, out_ref = refs
    count = len(row_refs)
    pair = lax.div(lax.axis_index("z"), 2)
    distances = sorted(range(count), key=lambda d: min(d, count - d))
    for distance, row_ref in zip(distances, row_refs):
        out_ref[lax.rem(pair + (count - distance), count)] = row_ref[...]


def apply_kernel(rows_ref, own_ref, other_ref, out_ref):
    half = own_ref.shape[1]
    dims = (((1,), (1,)), ((), ()))
    applied = lax.dot_general(rows_ref[:, :half], own_ref[...], dims, preferred_element_type=jnp.float32)
    applied += lax.dot_general(rows_ref[:, half:], other_ref[...], dims, preferred_element_type=jnp.float32)
    out_ref[...] = applied.astype(jnp.bfloat16).reshape(out_ref.shape)


def swapped(array):
    return lax.ppermute(array, "core", [(0, 1), (1, 0)])


def summed(pieces, params):
    return pl.pallas_call(
        sum_kernel,
        in_specs=[pl.BlockSpec(memory_space=pltpu.VMEM)],
        out_specs=pl.BlockSpec(memory_space=pltpu.VMEM),
        out_shape=jax.ShapeDtypeStruct(pieces.shape[1:], pieces.dtype),
        cost_estimate=pl.CostEstimate(flops=pieces.size, bytes_accessed=3 * pieces.size, transcendentals=0),
        compiler_params=params,
    )(pieces)


def stages(legendre, vectors, panel_orders, cycle_span, cycle_weight):
    orders, degrees, cycles = legendre.shape
    vecs = vectors.shape[2]
    panels = panel_orders.shape[0]
    half = cycles // 2
    pairs = orders * degrees
    vmem = pl.BlockSpec(memory_space=pltpu.VMEM)
    smem = pl.BlockSpec(memory_space=pltpu.SMEM)
    bf16 = jnp.bfloat16
    params = pltpu.CompilerParams(vmem_limit_bytes=24 * 1024 * 1024)

    other_tables = swapped(legendre)
    other_vectors = swapped(vectors)
    picks = pl.pallas_call(
        picks_kernel,
        in_specs=[smem, pl.BlockSpec(memory_space=pltpu.HBM)],
        out_specs=vmem,
        out_shape=jax.ShapeDtypeStruct((panels, lax.axis_size("yl"), degrees, cycles), bf16),
        scratch_shapes=[pltpu.SemaphoreType.DMA((panels, lax.axis_size("yl")))],
        cost_estimate=pl.CostEstimate(flops=1_000_000, bytes_accessed=400_000, transcendentals=0),
        compiler_params=pltpu.CompilerParams(vmem_limit_bytes=60 * 1024 * 1024),
    )(panel_orders, legendre)
    picked = lax.all_to_all(picks.reshape(-1, degrees, cycles), ROW_PAIR, 0, 0, tiled=True)

    partial = pl.pallas_call(
        panel_kernel,
        in_specs=[smem] + [vmem] * 6,
        out_specs=pl.BlockSpec(memory_space=pltpu.HBM),
        out_shape=jax.ShapeDtypeStruct((panels, vecs, half), bf16),
        scratch_shapes=[
            pltpu.VMEM((panels, orders, half), jnp.float32),
            pltpu.VMEM((4, panels, half), jnp.float32),
            pltpu.VMEM((2 * pairs // 256, 256 // degrees, degrees, half), bf16),
            pltpu.VMEM((2 * pairs // 256, vecs, 256), bf16),
            pltpu.VMEM((panels, vecs, half), bf16),
            pltpu.SemaphoreType.DMA,
        ],
        cost_estimate=pl.CostEstimate(
            flops=2 * panels * vecs * half * 2 * pairs, bytes_accessed=3_500_000, transcendentals=0
        ),
        compiler_params=params,
    )(
        panel_orders,
        cycle_span.T,
        cycle_weight.reshape(1, cycles),
        legendre,
        other_tables,
        vectors,
        other_vectors,
    )

    rows = pl.pallas_call(
        rows_kernel,
        in_specs=[smem, vmem],
        out_specs=vmem,
        out_shape=jax.ShapeDtypeStruct(picks.shape[1:], bf16),
        cost_estimate=pl.CostEstimate(flops=500_000, bytes_accessed=300_000, transcendentals=0),
        compiler_params=params,
    )(panel_orders, picked)
    count = lax.axis_size("z")
    paired = lax.ppermute(rows, "z", [(i, i ^ 1) for i in range(count)])
    joined = pl.pallas_call(
        join_kernel,
        in_specs=[vmem] * 2,
        out_specs=vmem,
        out_shape=jax.ShapeDtypeStruct((2, *rows.shape), bf16),
        cost_estimate=pl.CostEstimate(flops=100_000, bytes_accessed=128_000, transcendentals=0),
        compiler_params=params,
    )(rows, paired)
    spread = [joined]
    for distance in sorted(range(2, count, 2), key=lambda d: min(d, count - d)):
        spread.append(lax.ppermute(joined, "z", [(i, (i + distance) % count) for i in range(count)]))
    panel_rows = pl.pallas_call(
        place_kernel,
        in_specs=[vmem] * len(spread),
        out_specs=vmem,
        out_shape=jax.ShapeDtypeStruct((len(spread), *joined.shape), bf16),
        cost_estimate=pl.CostEstimate(flops=500_000, bytes_accessed=500_000, transcendentals=0),
        compiler_params=params,
    )(*spread).reshape(-1, cycles)

    pieces = lax.all_to_all(partial, ROW, 0, 0, tiled=True)
    own = summed(pieces, params)
    other = swapped(own)
    applied = pl.pallas_call(
        apply_kernel,
        in_specs=[vmem] * 3,
        out_specs=vmem,
        out_shape=jax.ShapeDtypeStruct((2 * count, degrees, vecs), bf16),
        cost_estimate=pl.CostEstimate(flops=2 * panel_rows.size * vecs, bytes_accessed=700_000, transcendentals=0),
        compiler_params=params,
    )(panel_rows, own, other)
    shares = lax.all_to_all(applied, PLANE, 0, 0, tiled=True)
    result = summed(shares, params)
    return result[:, None, :]


def solution(mesh):
    axes = Mesh(mesh.devices.reshape(2, 4, 8, 2, 2), ROW + COL)
    in_specs = (P(ROW, COL, None), P(ROW, COL, None), P(), P(), P())
    out_specs = P(COL, ROW, None)
    return jax.shard_map(stages, mesh=axes, in_specs=in_specs, out_specs=out_specs, check_vma=False)
```

```python
import math

import jax
import jax.numpy as jnp
from jax import lax
from jax.experimental import pallas as pl
from jax.experimental.pallas import tpu as pltpu
from jax.sharding import Mesh, PartitionSpec as P


NPHI = 2048
CELL = 2.0 * math.pi / NPHI
ROW = ("yh", "x")
COL = ("z", "yl", "core")
PLANE = ("z", "yl")
ROW_PAIR = ("yh", "x", "yl")


def sine_of_angle(x):
    square = x * x
    value = jnp.float32(-1.0 / 39916800.0)
    for term in (1.0 / 362880.0, -1.0 / 5040.0, 1.0 / 120.0, -1.0 / 6.0, 1.0):
        value = value * square + jnp.float32(term)
    return value * x


def sine_of_cells(cells):
    shifted = cells + NPHI // 4
    centred = (shifted & (NPHI // 2 - 1)) - NPHI // 4
    value = sine_of_angle(centred.astype(jnp.float32) * jnp.float32(CELL))
    return jnp.where((shifted & (NPHI // 2)) == 0, value, -value)


def half_denominator(wavenumber):
    angle = wavenumber.astype(jnp.float32) * jnp.float32(math.pi / NPHI)
    sine = 2.0 * sine_of_angle(angle)
    zero = wavenumber == 0
    return jnp.where(zero, 0.0, jnp.float32(CELL) / jnp.where(zero, 1.0, sine))


def picks_kernel(orders_ref, leg_ref, picks_ref, rows, sems):
    panels, sharers, degrees, cycles = picks_ref.shape
    orders = leg_ref.shape[0]
    half = cycles // 2
    first_order = lax.axis_index(ROW) * orders
    core = lax.axis_index("core")
    own = pl.ds(pl.multiple_of(core * half, half), half)
    other = pl.ds(pl.multiple_of((1 - core) * half, half), half)
    copies = []
    for p in range(panels):
        place = jnp.clip(orders_ref[p] - first_order, 0, orders - 1)
        copies.append(pltpu.make_async_copy(leg_ref.at[place], rows.at[p], sems.at[p]))
        copies[p].start()
    degree = lax.broadcasted_iota(jnp.int32, (degrees, half), 0) + lax.axis_index(COL) * degrees
    for p in range(panels):
        panel = orders_ref[p]
        held = (panel >= first_order) & (panel < first_order + orders)
        kept = degree >= jnp.where(held, panel, orders * lax.axis_size(ROW))
        copies[p].wait()
        for lanes, part in ((own, slice(0, half)), (other, slice(half, cycles))):
            pick = jnp.where(kept, rows[p, :, lanes].astype(jnp.float32), 0.0).astype(jnp.bfloat16)
            for sharer in range(sharers):
                picks_ref[p, sharer, :, part] = pick


def fill_coefs(orders_ref, span_ref, weight_ref, coefs, sides):
    panels, orders, half = coefs.shape
    first_order = lax.axis_index(ROW) * orders
    own = pl.ds(pl.multiple_of(lax.axis_index("core") * half, half), half)
    start, stop = span_ref[0:1, own], span_ref[1:2, own]
    weight = 0.5 * weight_ref[0:1, own]
    width = weight * (jnp.float32(CELL) * (stop - start).astype(jnp.float32))
    quarter = NPHI // 4
    sublane = lax.broadcasted_iota(jnp.int32, (panels, half), 0)
    lane = lax.broadcasted_iota(jnp.int32, (orders, 128), 1)
    panel_row, panel_lane = jnp.zeros_like(sublane), jnp.zeros_like(lane)
    for p in range(panels):
        panel_row = jnp.where(sublane == p, orders_ref[p], panel_row)
        panel_lane = jnp.where(lane == p, orders_ref[p], panel_lane)
    sides[0] = weight * sine_of_cells(panel_row * stop)
    sides[1] = weight * sine_of_cells(panel_row * start)
    sides[2] = weight * sine_of_cells(panel_row * stop + quarter)
    sides[3] = weight * sine_of_cells(panel_row * start + quarter)
    order = lax.broadcasted_iota(jnp.int32, (orders, half), 0) + first_order
    sin_stop, cos_stop = sine_of_cells(order * stop), sine_of_cells(order * stop + quarter)
    sin_start, cos_start = sine_of_cells(order * start), sine_of_cells(order * start + quarter)
    column = lax.broadcasted_iota(jnp.int32, (orders, 128), 0) + first_order
    over_sum, over_gap = half_denominator(panel_lane + column), half_denominator(panel_lane - column)
    even, odd = over_sum + over_gap, over_sum - over_gap
    for p in range(panels):
        at = slice(p, p + 1)
        coefs[p] = even[:, at] * (sides[0, at] * cos_stop - sides[1, at] * cos_start) + odd[:, at] * (
            sides[2, at] * sin_stop - sides[3, at] * sin_start
        )
    for p in range(panels):
        panel = orders_ref[p]
        held = (panel >= first_order) & (panel < first_order + orders)
        zeros = jnp.where(held, jnp.where(panel == 0, 2.0, 1.0), 0.0)
        at = pl.ds(jnp.clip(panel - first_order, 0, orders - 1), 1)
        coefs[p, at, :] = coefs[p, at, :] + zeros * width


def panel_kernel(orders_ref, span_ref, weight_ref, own_t_ref, other_t_ref, own_v_ref, other_v_ref, out_ref, *scratch):
    coefs, sides, tables, turned, sums, sem = scratch
    panels, orders, half = coefs.shape
    degrees, vecs = own_v_ref.shape[1:]
    block = 256 // degrees
    core = lax.axis_index("core")
    lanes = pl.ds(pl.multiple_of(core * half, half), half)
    first_order = lax.axis_index(ROW) * orders
    pair_degree = lax.axis_index(PLANE) * (2 * degrees)
    degree = lax.broadcasted_iota(jnp.int32, (degrees, half), 0)
    fill_coefs(orders_ref, span_ref, weight_ref, coefs, sides)
    blocks = []
    for t_ref, v_ref, offset in ((own_t_ref, own_v_ref, core), (other_t_ref, other_v_ref, 1 - core)):
        gap = degree + (pair_degree + offset * degrees - first_order)
        blocks += [(t_ref, v_ref, gap, first) for first in range(0, orders, block)]
    for p in range(panels):
        total = None
        for index, (t_ref, v_ref, gap, first) in enumerate(blocks):
            if p == 0:
                for i in range(block):
                    table = t_ref[first + i, :, lanes].astype(jnp.float32)
                    tables[index, i] = jnp.where(gap >= first + i, table, 0.0).astype(jnp.bfloat16)
                turned[index] = v_ref[first : first + block].reshape(block * degrees, vecs).T
            rows = []
            for i in range(block):
                coef = jnp.broadcast_to(coefs[p, pl.ds(first + i, 1), :], (degrees, half))
                rows.append(coef.astype(jnp.bfloat16) * tables[index, i])
            part = jnp.dot(turned[index], jnp.concatenate(rows, axis=0), preferred_element_type=jnp.float32)
            total = part if total is None else total + part
        sums[p] = total.astype(jnp.bfloat16)
    store = pltpu.make_async_copy(sums, out_ref, sem)
    store.start()
    store.wait()


def join_kernel(own_ref, other_ref, out_ref):
    mine = lax.rem(lax.axis_index("z"), 2)
    out_ref[mine] = own_ref[...]
    out_ref[1 - mine] = other_ref[...]


def place_kernel(*refs):
    *row_refs, out_ref = refs
    count = len(row_refs)
    pair = lax.div(lax.axis_index("z"), 2)
    distances = sorted(range(count), key=lambda d: min(d, count - d))
    for distance, row_ref in zip(distances, row_refs):
        out_ref[lax.rem(pair + (count - distance), count)] = row_ref[...]


def apply_kernel(rows_ref, own_ref, other_ref, out_ref):
    half = own_ref.shape[1]
    dims = (((1,), (1,)), ((), ()))
    applied = lax.dot_general(rows_ref[:, :half], own_ref[...], dims, preferred_element_type=jnp.float32)
    applied += lax.dot_general(rows_ref[:, half:], other_ref[...], dims, preferred_element_type=jnp.float32)
    out_ref[...] = applied.astype(jnp.bfloat16).reshape(out_ref.shape)


def finish_kernel(shares_ref, out_ref):
    count, _, width = shares_ref.shape
    sharers = out_ref.shape[1] // width
    for sharer in range(sharers):
        terms = [shares_ref[i].astype(jnp.float32) for i in range(sharer, count, sharers)]
        while len(terms) > 1:
            terms = [sum(terms[i : i + 2]) for i in range(0, len(terms), 2)]
        out_ref[:, sharer * width : (sharer + 1) * width] = terms[0].astype(jnp.bfloat16)


def swapped(array):
    return lax.ppermute(array, "core", [(0, 1), (1, 0)])


def stages(legendre, vectors, panel_orders, cycle_span, cycle_weight):
    orders, degrees, cycles = legendre.shape
    vecs = vectors.shape[2]
    panels = panel_orders.shape[0]
    half = cycles // 2
    pairs = orders * degrees
    vmem = pl.BlockSpec(memory_space=pltpu.VMEM)
    smem = pl.BlockSpec(memory_space=pltpu.SMEM)
    bf16 = jnp.bfloat16
    params = pltpu.CompilerParams(vmem_limit_bytes=24 * 1024 * 1024)

    other_tables = swapped(legendre)
    other_vectors = swapped(vectors)
    picks = pl.pallas_call(
        picks_kernel,
        in_specs=[smem, pl.BlockSpec(memory_space=pltpu.HBM)],
        out_specs=vmem,
        out_shape=jax.ShapeDtypeStruct((panels, lax.axis_size("yl"), degrees, cycles), bf16),
        scratch_shapes=[
            pltpu.VMEM((panels, degrees, cycles), bf16),
            pltpu.SemaphoreType.DMA((panels,)),
        ],
        cost_estimate=pl.CostEstimate(flops=1_000_000, bytes_accessed=400_000, transcendentals=0),
        compiler_params=pltpu.CompilerParams(vmem_limit_bytes=60 * 1024 * 1024),
    )(panel_orders, legendre)
    picked = lax.all_to_all(picks.reshape(-1, degrees, cycles), ROW_PAIR, 0, 0, tiled=True)

    partial = pl.pallas_call(
        panel_kernel,
        in_specs=[smem] + [vmem] * 6,
        out_specs=pl.BlockSpec(memory_space=pltpu.HBM),
        out_shape=jax.ShapeDtypeStruct((panels, vecs, half), bf16),
        scratch_shapes=[
            pltpu.VMEM((panels, orders, half), jnp.float32),
            pltpu.VMEM((4, panels, half), jnp.float32),
            pltpu.VMEM((2 * pairs // 256, 256 // degrees, degrees, half), bf16),
            pltpu.VMEM((2 * pairs // 256, vecs, 256), bf16),
            pltpu.VMEM((panels, vecs, half), bf16),
            pltpu.SemaphoreType.DMA,
        ],
        cost_estimate=pl.CostEstimate(
            flops=2 * panels * vecs * half * 2 * pairs, bytes_accessed=3_500_000, transcendentals=0
        ),
        compiler_params=params,
    )(
        panel_orders,
        cycle_span.T,
        cycle_weight.reshape(1, cycles),
        legendre,
        other_tables,
        vectors,
        other_vectors,
    )

    rows = jnp.sum(picked.reshape(picks.shape).astype(jnp.float32), axis=0).astype(bf16)
    count = lax.axis_size("z")
    paired = lax.ppermute(rows, "z", [(i, i ^ 1) for i in range(count)])
    joined = pl.pallas_call(
        join_kernel,
        in_specs=[vmem] * 2,
        out_specs=vmem,
        out_shape=jax.ShapeDtypeStruct((2, *rows.shape), bf16),
        cost_estimate=pl.CostEstimate(flops=100_000, bytes_accessed=128_000, transcendentals=0),
        compiler_params=params,
    )(rows, paired)
    spread = [joined]
    for distance in sorted(range(2, count, 2), key=lambda d: min(d, count - d)):
        spread.append(lax.ppermute(joined, "z", [(i, (i + distance) % count) for i in range(count)]))
    panel_rows = pl.pallas_call(
        place_kernel,
        in_specs=[vmem] * len(spread),
        out_specs=vmem,
        out_shape=jax.ShapeDtypeStruct((len(spread), *joined.shape), bf16),
        cost_estimate=pl.CostEstimate(flops=500_000, bytes_accessed=500_000, transcendentals=0),
        compiler_params=params,
    )(*spread).reshape(-1, cycles)

    halves = partial.reshape(-1, vecs // lax.axis_size("yl"), half)
    pieces = lax.all_to_all(halves, ROW_PAIR, 0, 0, tiled=True)
    own = jnp.sum(pieces.astype(jnp.float32), axis=0).astype(bf16)
    other = swapped(own)
    applied = pl.pallas_call(
        apply_kernel,
        in_specs=[vmem] * 3,
        out_specs=vmem,
        out_shape=jax.ShapeDtypeStruct((2 * count, degrees, own.shape[0]), bf16),
        cost_estimate=pl.CostEstimate(flops=2 * panel_rows.size * own.shape[0], bytes_accessed=700_000, transcendentals=0),
        compiler_params=params,
    )(panel_rows, own, other)
    shares = lax.all_to_all(applied, PLANE, 0, 0, tiled=True)
    result = pl.pallas_call(
        finish_kernel,
        in_specs=[vmem],
        out_specs=vmem,
        out_shape=jax.ShapeDtypeStruct((degrees, vecs), bf16),
        cost_estimate=pl.CostEstimate(flops=shares.size, bytes_accessed=200_000, transcendentals=0),
        compiler_params=params,
    )(shares)
    return result[:, None, :]


def solution(mesh):
    axes = Mesh(mesh.devices.reshape(2, 4, 8, 2, 2), ROW + COL)
    in_specs = (P(ROW, COL, None), P(ROW, COL, None), P(), P(), P())
    out_specs = P(COL, ROW, None)
    return jax.shard_map(stages, mesh=axes, in_specs=in_specs, out_specs=out_specs, check_vma=False)
```

```python
import math

import jax
import jax.numpy as jnp
from jax import lax
from jax.experimental import pallas as pl
from jax.experimental.pallas import tpu as pltpu
from jax.sharding import Mesh, PartitionSpec as P


NPHI = 2048
CELL = 2.0 * math.pi / NPHI
ROW = ("yh", "x")
COL = ("z", "yl", "core")
PLANE = ("z", "yl")
ROW_PAIR = ("yh", "x", "yl")


def sine_of_angle(x):
    square = x * x
    value = jnp.float32(-1.0 / 39916800.0)
    for term in (1.0 / 362880.0, -1.0 / 5040.0, 1.0 / 120.0, -1.0 / 6.0, 1.0):
        value = value * square + jnp.float32(term)
    return value * x


def sine_of_cells(cells):
    shifted = cells + NPHI // 4
    centred = (shifted & (NPHI // 2 - 1)) - NPHI // 4
    value = sine_of_angle(centred.astype(jnp.float32) * jnp.float32(CELL))
    return jnp.where((shifted & (NPHI // 2)) == 0, value, -value)


def half_denominator(wavenumber):
    angle = wavenumber.astype(jnp.float32) * jnp.float32(math.pi / NPHI)
    sine = 2.0 * sine_of_angle(angle)
    zero = wavenumber == 0
    return jnp.where(zero, 0.0, jnp.float32(CELL) / jnp.where(zero, 1.0, sine))


def picks_kernel(orders_ref, leg_ref, picks_ref, panel_orders, tables, sems):
    panels, sharers, degrees, cycles = picks_ref.shape
    orders = leg_ref.shape[0]
    half = cycles // 2
    first_order = lax.axis_index(ROW) * orders
    core = lax.axis_index("core")
    own = pl.ds(pl.multiple_of(core * half, half), half)
    other = pl.ds(pl.multiple_of((1 - core) * half, half), half)
    copies = [
        pltpu.make_async_copy(orders_ref, panel_orders, sems.at[0]),
        pltpu.make_async_copy(leg_ref, tables, sems.at[1]),
    ]
    for copy in copies:
        copy.start()
    degree = lax.broadcasted_iota(jnp.int32, (degrees, half), 0) + lax.axis_index(COL) * degrees
    for copy in copies:
        copy.wait()
    for p in range(panels):
        panel = panel_orders[p]
        held = (panel >= first_order) & (panel < first_order + orders)
        place = jnp.clip(panel - first_order, 0, orders - 1)
        kept = degree >= jnp.where(held, panel, orders * lax.axis_size(ROW))
        for lanes, part in ((own, slice(0, half)), (other, slice(half, cycles))):
            pick = jnp.where(kept, tables[place, :, lanes].astype(jnp.float32), 0.0).astype(jnp.bfloat16)
            for sharer in range(sharers):
                picks_ref[p, sharer, :, part] = pick


def fill_coefs(orders_ref, span_ref, weight_ref, coefs, sides):
    panels, orders, half = coefs.shape
    first_order = lax.axis_index(ROW) * orders
    own = pl.ds(pl.multiple_of(lax.axis_index("core") * half, half), half)
    start, stop = span_ref[0:1, own], span_ref[1:2, own]
    weight = 0.5 * weight_ref[0:1, own]
    width = weight * (jnp.float32(CELL) * (stop - start).astype(jnp.float32))
    quarter = NPHI // 4
    sublane = lax.broadcasted_iota(jnp.int32, (panels, half), 0)
    lane = lax.broadcasted_iota(jnp.int32, (orders, 128), 1)
    panel_row, panel_lane = jnp.zeros_like(sublane), jnp.zeros_like(lane)
    for p in range(panels):
        panel_row = jnp.where(sublane == p, orders_ref[p], panel_row)
        panel_lane = jnp.where(lane == p, orders_ref[p], panel_lane)
    sides[0] = weight * sine_of_cells(panel_row * stop)
    sides[1] = weight * sine_of_cells(panel_row * start)
    sides[2] = weight * sine_of_cells(panel_row * stop + quarter)
    sides[3] = weight * sine_of_cells(panel_row * start + quarter)
    order = lax.broadcasted_iota(jnp.int32, (orders, half), 0) + first_order
    sin_stop, cos_stop = sine_of_cells(order * stop), sine_of_cells(order * stop + quarter)
    sin_start, cos_start = sine_of_cells(order * start), sine_of_cells(order * start + quarter)
    column = lax.broadcasted_iota(jnp.int32, (orders, 128), 0) + first_order
    over_sum, over_gap = half_denominator(panel_lane + column), half_denominator(panel_lane - column)
    even, odd = over_sum + over_gap, over_sum - over_gap
    for p in range(panels):
        at = slice(p, p + 1)
        coefs[p] = even[:, at] * (sides[0, at] * cos_stop - sides[1, at] * cos_start) + odd[:, at] * (
            sides[2, at] * sin_stop - sides[3, at] * sin_start
        )
    for p in range(panels):
        panel = orders_ref[p]
        held = (panel >= first_order) & (panel < first_order + orders)
        zeros = jnp.where(held, jnp.where(panel == 0, 2.0, 1.0), 0.0)
        at = pl.ds(jnp.clip(panel - first_order, 0, orders - 1), 1)
        coefs[p, at, :] = coefs[p, at, :] + zeros * width


def panel_kernel(orders_ref, span_ref, weight_ref, own_t_ref, other_t_ref, own_v_ref, other_v_ref, out_ref, *scratch):
    coefs, sides, tables, turned, sums, sem = scratch
    panels, orders, half = coefs.shape
    degrees, vecs = own_v_ref.shape[1:]
    block = 256 // degrees
    core = lax.axis_index("core")
    lanes = pl.ds(pl.multiple_of(core * half, half), half)
    first_order = lax.axis_index(ROW) * orders
    pair_degree = lax.axis_index(PLANE) * (2 * degrees)
    degree = lax.broadcasted_iota(jnp.int32, (degrees, half), 0)
    fill_coefs(orders_ref, span_ref, weight_ref, coefs, sides)
    blocks = []
    for t_ref, v_ref, offset in ((own_t_ref, own_v_ref, core), (other_t_ref, other_v_ref, 1 - core)):
        gap = degree + (pair_degree + offset * degrees - first_order)
        blocks += [(t_ref, v_ref, gap, first) for first in range(0, orders, block)]
    for p in range(panels):
        total = None
        for index, (t_ref, v_ref, gap, first) in enumerate(blocks):
            if p == 0:
                for i in range(block):
                    table = t_ref[first + i, :, lanes].astype(jnp.float32)
                    tables[index, i] = jnp.where(gap >= first + i, table, 0.0).astype(jnp.bfloat16)
                turned[index] = v_ref[first : first + block].reshape(block * degrees, vecs).T
            rows = []
            for i in range(block):
                coef = jnp.broadcast_to(coefs[p, pl.ds(first + i, 1), :], (degrees, half))
                rows.append(coef.astype(jnp.bfloat16) * tables[index, i])
            part = jnp.dot(turned[index], jnp.concatenate(rows, axis=0), preferred_element_type=jnp.float32)
            total = part if total is None else total + part
        sums[p] = total.astype(jnp.bfloat16)
    store = pltpu.make_async_copy(sums, out_ref, sem)
    store.start()
    store.wait()


def join_kernel(own_ref, other_ref, out_ref):
    mine = lax.rem(lax.axis_index("z"), 2)
    out_ref[mine] = own_ref[...]
    out_ref[1 - mine] = other_ref[...]


def place_kernel(*refs):
    *row_refs, out_ref = refs
    count = len(row_refs)
    pair = lax.div(lax.axis_index("z"), 2)
    distances = sorted(range(count), key=lambda d: min(d, count - d))
    for distance, row_ref in zip(distances, row_refs):
        out_ref[lax.rem(pair + (count - distance), count)] = row_ref[...]


def apply_kernel(rows_ref, own_ref, other_ref, out_ref):
    half = own_ref.shape[1]
    dims = (((1,), (1,)), ((), ()))
    applied = lax.dot_general(rows_ref[:, :half], own_ref[...], dims, preferred_element_type=jnp.float32)
    applied += lax.dot_general(rows_ref[:, half:], other_ref[...], dims, preferred_element_type=jnp.float32)
    out_ref[...] = applied.astype(jnp.bfloat16).reshape(out_ref.shape)


def finish_kernel(shares_ref, out_ref):
    count, _, width = shares_ref.shape
    sharers = out_ref.shape[1] // width
    for sharer in range(sharers):
        terms = [shares_ref[i].astype(jnp.float32) for i in range(sharer, count, sharers)]
        while len(terms) > 1:
            terms = [sum(terms[i : i + 2]) for i in range(0, len(terms), 2)]
        out_ref[:, sharer * width : (sharer + 1) * width] = terms[0].astype(jnp.bfloat16)


def swapped(array):
    return lax.ppermute(array, "core", [(0, 1), (1, 0)])


def stages(legendre, vectors, panel_orders, cycle_span, cycle_weight):
    orders, degrees, cycles = legendre.shape
    vecs = vectors.shape[2]
    panels = panel_orders.shape[0]
    half = cycles // 2
    pairs = orders * degrees
    vmem = pl.BlockSpec(memory_space=pltpu.VMEM)
    smem = pl.BlockSpec(memory_space=pltpu.SMEM)
    bf16 = jnp.bfloat16
    params = pltpu.CompilerParams(vmem_limit_bytes=24 * 1024 * 1024)

    other_tables = swapped(legendre)
    other_vectors = swapped(vectors)
    picks = pl.pallas_call(
        picks_kernel,
        in_specs=[pl.BlockSpec(memory_space=pltpu.HBM)] * 2,
        out_specs=vmem,
        out_shape=jax.ShapeDtypeStruct((panels, lax.axis_size("yl"), degrees, cycles), bf16),
        scratch_shapes=[
            pltpu.SMEM((panels,), jnp.int32),
            pltpu.VMEM((orders, degrees, cycles), bf16),
            pltpu.SemaphoreType.DMA((2,)),
        ],
        cost_estimate=pl.CostEstimate(flops=1_000_000, bytes_accessed=400_000, transcendentals=0),
        compiler_params=pltpu.CompilerParams(vmem_limit_bytes=60 * 1024 * 1024),
    )(panel_orders, legendre)
    picked = lax.all_to_all(picks.reshape(-1, degrees, cycles), ROW_PAIR, 0, 0, tiled=True)

    partial = pl.pallas_call(
        panel_kernel,
        in_specs=[smem] + [vmem] * 6,
        out_specs=pl.BlockSpec(memory_space=pltpu.HBM),
        out_shape=jax.ShapeDtypeStruct((panels, vecs, half), bf16),
        scratch_shapes=[
            pltpu.VMEM((panels, orders, half), jnp.float32),
            pltpu.VMEM((4, panels, half), jnp.float32),
            pltpu.VMEM((2 * pairs // 256, 256 // degrees, degrees, half), bf16),
            pltpu.VMEM((2 * pairs // 256, vecs, 256), bf16),
            pltpu.VMEM((panels, vecs, half), bf16),
            pltpu.SemaphoreType.DMA,
        ],
        cost_estimate=pl.CostEstimate(
            flops=2 * panels * vecs * half * 2 * pairs, bytes_accessed=3_500_000, transcendentals=0
        ),
        compiler_params=params,
    )(
        panel_orders,
        cycle_span.T,
        cycle_weight.reshape(1, cycles),
        legendre,
        other_tables,
        vectors,
        other_vectors,
    )

    rows = jnp.sum(picked.reshape(picks.shape).astype(jnp.float32), axis=0).astype(bf16)
    count = lax.axis_size("z")
    paired = lax.ppermute(rows, "z", [(i, i ^ 1) for i in range(count)])
    joined = pl.pallas_call(
        join_kernel,
        in_specs=[vmem] * 2,
        out_specs=vmem,
        out_shape=jax.ShapeDtypeStruct((2, *rows.shape), bf16),
        cost_estimate=pl.CostEstimate(flops=100_000, bytes_accessed=128_000, transcendentals=0),
        compiler_params=params,
    )(rows, paired)
    spread = [joined]
    for distance in sorted(range(2, count, 2), key=lambda d: min(d, count - d)):
        spread.append(lax.ppermute(joined, "z", [(i, (i + distance) % count) for i in range(count)]))
    panel_rows = pl.pallas_call(
        place_kernel,
        in_specs=[vmem] * len(spread),
        out_specs=vmem,
        out_shape=jax.ShapeDtypeStruct((len(spread), *joined.shape), bf16),
        cost_estimate=pl.CostEstimate(flops=500_000, bytes_accessed=500_000, transcendentals=0),
        compiler_params=params,
    )(*spread).reshape(-1, cycles)

    halves = partial.reshape(-1, vecs // lax.axis_size("yl"), half)
    pieces = lax.all_to_all(halves, ROW_PAIR, 0, 0, tiled=True)
    own = jnp.sum(pieces.astype(jnp.float32), axis=0).astype(bf16)
    other = swapped(own)
    applied = pl.pallas_call(
        apply_kernel,
        in_specs=[vmem] * 3,
        out_specs=vmem,
        out_shape=jax.ShapeDtypeStruct((2 * count, degrees, own.shape[0]), bf16),
        cost_estimate=pl.CostEstimate(flops=2 * panel_rows.size * own.shape[0], bytes_accessed=700_000, transcendentals=0),
        compiler_params=params,
    )(panel_rows, own, other)
    shares = lax.all_to_all(applied, PLANE, 0, 0, tiled=True)
    result = pl.pallas_call(
        finish_kernel,
        in_specs=[vmem],
        out_specs=vmem,
        out_shape=jax.ShapeDtypeStruct((degrees, vecs), bf16),
        cost_estimate=pl.CostEstimate(flops=shares.size, bytes_accessed=200_000, transcendentals=0),
        compiler_params=params,
    )(shares)
    return result[:, None, :]


def solution(mesh):
    axes = Mesh(mesh.devices.reshape(2, 4, 8, 2, 2), ROW + COL)
    in_specs = (P(ROW, COL, None), P(ROW, COL, None), P(), P(), P())
    out_specs = P(COL, ROW, None)
    return jax.shard_map(stages, mesh=axes, in_specs=in_specs, out_specs=out_specs, check_vma=False)
```

```python
import math

import jax
import jax.numpy as jnp
from jax import lax
from jax.experimental import pallas as pl
from jax.experimental.pallas import tpu as pltpu
from jax.sharding import Mesh, PartitionSpec as P


NPHI = 2048
CELL = 2.0 * math.pi / NPHI
ROW = ("yh", "x")
COL = ("z", "yl", "core")
PLANE = ("z", "yl")
ROW_PAIR = ("yh", "x", "yl")


def sine_of_angle(x):
    square = x * x
    value = jnp.float32(-1.0 / 39916800.0)
    for term in (1.0 / 362880.0, -1.0 / 5040.0, 1.0 / 120.0, -1.0 / 6.0, 1.0):
        value = value * square + jnp.float32(term)
    return value * x


def sine_of_cells(cells):
    shifted = cells + NPHI // 4
    centred = (shifted & (NPHI // 2 - 1)) - NPHI // 4
    value = sine_of_angle(centred.astype(jnp.float32) * jnp.float32(CELL))
    return jnp.where((shifted & (NPHI // 2)) == 0, value, -value)


def half_denominator(wavenumber):
    angle = wavenumber.astype(jnp.float32) * jnp.float32(math.pi / NPHI)
    sine = 2.0 * sine_of_angle(angle)
    zero = wavenumber == 0
    return jnp.where(zero, 0.0, jnp.float32(CELL) / jnp.where(zero, 1.0, sine))


def picks_kernel(orders_ref, leg_ref, picks_ref, panel_orders, tables, sems):
    panels, sharers, degrees, cycles = picks_ref.shape
    orders = leg_ref.shape[0]
    half = cycles // 2
    first_order = lax.axis_index(ROW) * orders
    core = lax.axis_index("core")
    own = pl.ds(pl.multiple_of(core * half, half), half)
    other = pl.ds(pl.multiple_of((1 - core) * half, half), half)
    copies = [pltpu.make_async_copy(orders_ref, panel_orders, sems.at[0])]
    share = orders // (sems.shape[0] - 1)
    for i in range(1, sems.shape[0]):
        copies.append(pltpu.make_async_copy(leg_ref.at[pl.ds((i - 1) * share, share)], tables.at[pl.ds((i - 1) * share, share)], sems.at[i]))
    for copy in copies:
        copy.start()
    degree = lax.broadcasted_iota(jnp.int32, (degrees, half), 0) + lax.axis_index(COL) * degrees
    for copy in copies:
        copy.wait()
    for p in range(panels):
        panel = panel_orders[p]
        held = (panel >= first_order) & (panel < first_order + orders)
        place = jnp.clip(panel - first_order, 0, orders - 1)
        kept = degree >= jnp.where(held, panel, orders * lax.axis_size(ROW))
        for lanes, part in ((own, slice(0, half)), (other, slice(half, cycles))):
            pick = jnp.where(kept, tables[place, :, lanes].astype(jnp.float32), 0.0).astype(jnp.bfloat16)
            for sharer in range(sharers):
                picks_ref[p, sharer, :, part] = pick


def fill_coefs(orders_ref, span_ref, weight_ref, coefs, sides):
    panels, orders, half = coefs.shape
    first_order = lax.axis_index(ROW) * orders
    own = pl.ds(pl.multiple_of(lax.axis_index("core") * half, half), half)
    start, stop = span_ref[0:1, own], span_ref[1:2, own]
    weight = 0.5 * weight_ref[0:1, own]
    width = weight * (jnp.float32(CELL) * (stop - start).astype(jnp.float32))
    quarter = NPHI // 4
    sublane = lax.broadcasted_iota(jnp.int32, (panels, half), 0)
    lane = lax.broadcasted_iota(jnp.int32, (orders, 128), 1)
    panel_row, panel_lane = jnp.zeros_like(sublane), jnp.zeros_like(lane)
    for p in range(panels):
        panel_row = jnp.where(sublane == p, orders_ref[p], panel_row)
        panel_lane = jnp.where(lane == p, orders_ref[p], panel_lane)
    sides[0] = weight * sine_of_cells(panel_row * stop)
    sides[1] = weight * sine_of_cells(panel_row * start)
    sides[2] = weight * sine_of_cells(panel_row * stop + quarter)
    sides[3] = weight * sine_of_cells(panel_row * start + quarter)
    order = lax.broadcasted_iota(jnp.int32, (orders, half), 0) + first_order
    sin_stop, cos_stop = sine_of_cells(order * stop), sine_of_cells(order * stop + quarter)
    sin_start, cos_start = sine_of_cells(order * start), sine_of_cells(order * start + quarter)
    column = lax.broadcasted_iota(jnp.int32, (orders, 128), 0) + first_order
    over_sum, over_gap = half_denominator(panel_lane + column), half_denominator(panel_lane - column)
    even, odd = over_sum + over_gap, over_sum - over_gap
    for p in range(panels):
        at = slice(p, p + 1)
        coefs[p] = even[:, at] * (sides[0, at] * cos_stop - sides[1, at] * cos_start) + odd[:, at] * (
            sides[2, at] * sin_stop - sides[3, at] * sin_start
        )
    for p in range(panels):
        panel = orders_ref[p]
        held = (panel >= first_order) & (panel < first_order + orders)
        zeros = jnp.where(held, jnp.where(panel == 0, 2.0, 1.0), 0.0)
        at = pl.ds(jnp.clip(panel - first_order, 0, orders - 1), 1)
        coefs[p, at, :] = coefs[p, at, :] + zeros * width


def panel_kernel(orders_ref, span_ref, weight_ref, own_t_ref, other_t_ref, own_v_ref, other_v_ref, out_ref, *scratch):
    coefs, sides, tables, turned, sums, sem = scratch
    panels, orders, half = coefs.shape
    degrees, vecs = own_v_ref.shape[1:]
    block = 256 // degrees
    core = lax.axis_index("core")
    lanes = pl.ds(pl.multiple_of(core * half, half), half)
    first_order = lax.axis_index(ROW) * orders
    pair_degree = lax.axis_index(PLANE) * (2 * degrees)
    degree = lax.broadcasted_iota(jnp.int32, (degrees, half), 0)
    fill_coefs(orders_ref, span_ref, weight_ref, coefs, sides)
    blocks = []
    for t_ref, v_ref, offset in ((own_t_ref, own_v_ref, core), (other_t_ref, other_v_ref, 1 - core)):
        gap = degree + (pair_degree + offset * degrees - first_order)
        blocks += [(t_ref, v_ref, gap, first) for first in range(0, orders, block)]
    for p in range(panels):
        total = None
        for index, (t_ref, v_ref, gap, first) in enumerate(blocks):
            if p == 0:
                for i in range(block):
                    table = t_ref[first + i, :, lanes].astype(jnp.float32)
                    tables[index, i] = jnp.where(gap >= first + i, table, 0.0).astype(jnp.bfloat16)
                turned[index] = v_ref[first : first + block].reshape(block * degrees, vecs).T
            rows = []
            for i in range(block):
                coef = jnp.broadcast_to(coefs[p, pl.ds(first + i, 1), :], (degrees, half))
                rows.append(coef.astype(jnp.bfloat16) * tables[index, i])
            part = jnp.dot(turned[index], jnp.concatenate(rows, axis=0), preferred_element_type=jnp.float32)
            total = part if total is None else total + part
        sums[p] = total.astype(jnp.bfloat16)
    store = pltpu.make_async_copy(sums, out_ref, sem)
    store.start()
    store.wait()


def join_kernel(own_ref, other_ref, out_ref):
    mine = lax.rem(lax.axis_index("z"), 2)
    out_ref[mine] = own_ref[...]
    out_ref[1 - mine] = other_ref[...]


def place_kernel(*refs):
    *row_refs, out_ref = refs
    count = len(row_refs)
    pair = lax.div(lax.axis_index("z"), 2)
    distances = sorted(range(count), key=lambda d: min(d, count - d))
    for distance, row_ref in zip(distances, row_refs):
        out_ref[lax.rem(pair + (count - distance), count)] = row_ref[...]


def apply_kernel(rows_ref, own_ref, other_ref, out_ref):
    half = own_ref.shape[1]
    dims = (((1,), (1,)), ((), ()))
    applied = lax.dot_general(rows_ref[:, :half], own_ref[...], dims, preferred_element_type=jnp.float32)
    applied += lax.dot_general(rows_ref[:, half:], other_ref[...], dims, preferred_element_type=jnp.float32)
    out_ref[...] = applied.astype(jnp.bfloat16).reshape(out_ref.shape)


def finish_kernel(shares_ref, out_ref):
    count, _, width = shares_ref.shape
    sharers = out_ref.shape[1] // width
    for sharer in range(sharers):
        terms = [shares_ref[i].astype(jnp.float32) for i in range(sharer, count, sharers)]
        while len(terms) > 1:
            terms = [sum(terms[i : i + 2]) for i in range(0, len(terms), 2)]
        out_ref[:, sharer * width : (sharer + 1) * width] = terms[0].astype(jnp.bfloat16)


def swapped(array):
    return lax.ppermute(array, "core", [(0, 1), (1, 0)])


def stages(legendre, vectors, panel_orders, cycle_span, cycle_weight):
    orders, degrees, cycles = legendre.shape
    vecs = vectors.shape[2]
    panels = panel_orders.shape[0]
    half = cycles // 2
    pairs = orders * degrees
    vmem = pl.BlockSpec(memory_space=pltpu.VMEM)
    smem = pl.BlockSpec(memory_space=pltpu.SMEM)
    bf16 = jnp.bfloat16
    params = pltpu.CompilerParams(vmem_limit_bytes=24 * 1024 * 1024)

    other_tables = swapped(legendre)
    other_vectors = swapped(vectors)
    picks = pl.pallas_call(
        picks_kernel,
        in_specs=[pl.BlockSpec(memory_space=pltpu.HBM)] * 2,
        out_specs=vmem,
        out_shape=jax.ShapeDtypeStruct((panels, lax.axis_size("yl"), degrees, cycles), bf16),
        scratch_shapes=[
            pltpu.SMEM((panels,), jnp.int32),
            pltpu.VMEM((orders, degrees, cycles), bf16),
            pltpu.SemaphoreType.DMA((5,)),
        ],
        cost_estimate=pl.CostEstimate(flops=1_000_000, bytes_accessed=400_000, transcendentals=0),
        compiler_params=pltpu.CompilerParams(vmem_limit_bytes=60 * 1024 * 1024),
    )(panel_orders, legendre)
    picked = lax.all_to_all(picks.reshape(-1, degrees, cycles), ROW_PAIR, 0, 0, tiled=True)

    partial = pl.pallas_call(
        panel_kernel,
        in_specs=[smem] + [vmem] * 6,
        out_specs=pl.BlockSpec(memory_space=pltpu.HBM),
        out_shape=jax.ShapeDtypeStruct((panels, vecs, half), bf16),
        scratch_shapes=[
            pltpu.VMEM((panels, orders, half), jnp.float32),
            pltpu.VMEM((4, panels, half), jnp.float32),
            pltpu.VMEM((2 * pairs // 256, 256 // degrees, degrees, half), bf16),
            pltpu.VMEM((2 * pairs // 256, vecs, 256), bf16),
            pltpu.VMEM((panels, vecs, half), bf16),
            pltpu.SemaphoreType.DMA,
        ],
        cost_estimate=pl.CostEstimate(
            flops=2 * panels * vecs * half * 2 * pairs, bytes_accessed=3_500_000, transcendentals=0
        ),
        compiler_params=params,
    )(
        panel_orders,
        cycle_span.T,
        cycle_weight.reshape(1, cycles),
        legendre,
        other_tables,
        vectors,
        other_vectors,
    )

    rows = jnp.sum(picked.reshape(picks.shape).astype(jnp.float32), axis=0).astype(bf16)
    count = lax.axis_size("z")
    paired = lax.ppermute(rows, "z", [(i, i ^ 1) for i in range(count)])
    joined = pl.pallas_call(
        join_kernel,
        in_specs=[vmem] * 2,
        out_specs=vmem,
        out_shape=jax.ShapeDtypeStruct((2, *rows.shape), bf16),
        cost_estimate=pl.CostEstimate(flops=100_000, bytes_accessed=128_000, transcendentals=0),
        compiler_params=params,
    )(rows, paired)
    spread = [joined]
    for distance in sorted(range(2, count, 2), key=lambda d: min(d, count - d)):
        spread.append(lax.ppermute(joined, "z", [(i, (i + distance) % count) for i in range(count)]))
    panel_rows = pl.pallas_call(
        place_kernel,
        in_specs=[vmem] * len(spread),
        out_specs=vmem,
        out_shape=jax.ShapeDtypeStruct((len(spread), *joined.shape), bf16),
        cost_estimate=pl.CostEstimate(flops=500_000, bytes_accessed=500_000, transcendentals=0),
        compiler_params=params,
    )(*spread).reshape(-1, cycles)

    halves = partial.reshape(-1, vecs // lax.axis_size("yl"), half)
    pieces = lax.all_to_all(halves, ROW_PAIR, 0, 0, tiled=True)
    own = jnp.sum(pieces.astype(jnp.float32), axis=0).astype(bf16)
    other = swapped(own)
    applied = pl.pallas_call(
        apply_kernel,
        in_specs=[vmem] * 3,
        out_specs=vmem,
        out_shape=jax.ShapeDtypeStruct((2 * count, degrees, own.shape[0]), bf16),
        cost_estimate=pl.CostEstimate(flops=2 * panel_rows.size * own.shape[0], bytes_accessed=700_000, transcendentals=0),
        compiler_params=params,
    )(panel_rows, own, other)
    shares = lax.all_to_all(applied, PLANE, 0, 0, tiled=True)
    result = pl.pallas_call(
        finish_kernel,
        in_specs=[vmem],
        out_specs=vmem,
        out_shape=jax.ShapeDtypeStruct((degrees, vecs), bf16),
        cost_estimate=pl.CostEstimate(flops=shares.size, bytes_accessed=200_000, transcendentals=0),
        compiler_params=params,
    )(shares)
    return result[:, None, :]


def solution(mesh):
    axes = Mesh(mesh.devices.reshape(2, 4, 8, 2, 2), ROW + COL)
    in_specs = (P(ROW, COL, None), P(ROW, COL, None), P(), P(), P())
    out_specs = P(COL, ROW, None)
    return jax.shard_map(stages, mesh=axes, in_specs=in_specs, out_specs=out_specs, check_vma=False)
```
